128 devices in a mesh: grp: 4 (over y), shard: 32 (over z, x, core).
Axes of the slice: x: 4, y: 4, z: 4, core: 2. Of those that a mesh axis runs over, the one named last changes fastest.
Arguments:
- bucket: int32 [786432], P(('grp', 'shard')), may hold values from 0 to 1048575
- label: int32 [786432], P(('grp', 'shard')), may hold values from 0 to 1
- group: int32 [786432], P(('grp', 'shard')), may hold values from 0 to 15
- group_weight: float32 [16], replicated, may hold values from 0.25 to 4
Outputs:
- tpr_curve: float32 [1048576], P('shard')
- precision_curve: float32 [1048576], P('shard')
- auroc: float32 [], replicated
- auprc: float32 [], replicated
The draws below stay inside these ranges and needn't reach their ends.
All inputs are finite; a program needn't handle non-finite values.
Results may differ from the reference program's by a relative error of at most 0.0003.
Values sent between devices are 32-bit elements; how exact they have to be, the bound alone decides.
No kernel may reach another device: no remote copies, remote signals or barrier semaphores. Data moves between devices by JAX's collectives and lax.ppermute only.
A program may use at most 64 MiB of HBM per device.

```python
import math
import jax
import jax.numpy as jnp
from jax import lax

BUCKETS = 1048576
GROUPS = 16
EXAMPLES = 786432


def joint_draw(key):
    inner = jax.random.fold_in(key, 7)
    first, second, third = jax.random.split(inner, 3)
    position = jnp.arange(EXAMPLES, dtype=jnp.int32)
    threshold = 100 + 300 * position // EXAMPLES
    clicks = (jax.random.randint(first, (EXAMPLES,), 0, 1000) < threshold).astype(jnp.int32)
    lower = jax.random.randint(second, (EXAMPLES,), 0, BUCKETS)
    upper = jax.random.randint(third, (EXAMPLES,), 0, BUCKETS)
    buckets = jnp.where(clicks == 1, jnp.maximum(lower, upper), lower).astype(jnp.int32)
    return (buckets, clicks)


def draw_bucket(key, part):
    return joint_draw(key)[0]


def draw_label(key, part):
    return joint_draw(key)[1]


def plant(drawn, rng, smallest, high):
    place = [jax.random.randint(jax.random.fold_in(rng, axis), (), 0, length) for axis, length in enumerate(drawn.shape)]
    longest = drawn.shape.index(max(drawn.shape))
    next_to = place[:longest] + [(place[longest] + 1) % drawn.shape[longest]] + place[longest + 1:]
    return drawn.at[tuple(place)].set(smallest).at[tuple(next_to)].set(high)


def setup_inputs(seed: int = 0) -> dict:
    seeds = jax.random.split(jax.random.key(seed), 5)
    bucket = draw_bucket(jax.random.fold_in(seeds[4], 71), 0)
    label = draw_label(jax.random.fold_in(seeds[4], 71), 0)
    group = plant(jax.random.randint(seeds[2], (EXAMPLES,), 0, GROUPS), jax.random.fold_in(seeds[2], 1), 0, GROUPS - 1).astype(jnp.int32)
    group_weight = jnp.clip(jnp.exp(jax.random.uniform(seeds[3], (GROUPS,), jnp.float32, math.log(0.25), math.log(4.0))), 0.25, 4.0)
    return {"bucket": bucket, "label": label, "group": group, "group_weight": group_weight}


def reference(bucket, label, group, group_weight):
    weight = group_weight[group]
    labels = label.astype(jnp.float32)
    positive_w = (weight * labels).astype(jnp.bfloat16)
    negative_w = (weight * (1.0 - labels)).astype(jnp.bfloat16)
    positive_w, negative_w = lax.optimization_barrier((positive_w, negative_w))
    pos_hist = jnp.zeros((BUCKETS,), jnp.float32).at[bucket].add(positive_w.astype(jnp.float32))
    neg_hist = jnp.zeros((BUCKETS,), jnp.float32).at[bucket].add(negative_w.astype(jnp.float32))
    true_pos = jnp.cumsum(pos_hist[::-1])[::-1]
    false_pos = jnp.cumsum(neg_hist[::-1])[::-1]
    total_pos = true_pos[0]
    total_neg = false_pos[0]
    tpr_curve = true_pos / total_pos
    precision_curve = true_pos / jnp.maximum(true_pos + false_pos, 1.0)
    auroc = jnp.sum(neg_hist * (2.0 * true_pos - pos_hist)) / (2.0 * total_pos * total_neg)
    auprc = jnp.sum(pos_hist * precision_curve) / total_pos
    return tpr_curve, precision_curve, auroc, auprc
```

```python
import jax
import jax.numpy as jnp
from jax import lax
from jax.experimental import pallas as pl
from jax.experimental.pallas import tpu as pltpu
from jax.sharding import PartitionSpec as P

LO = 256
BLOCK = 1024
HI = 4096

AXES = ("grp", "shard")
LANES = 128
RANGES = 128
RANGE_BITS = 13
ROWS = 64
CAP = 126
NT = (((1,), (1,)), ((), ()))
NN = (((1,), (0,)), ((), ()))
HIGHEST = lax.Precision.HIGHEST


def copy_for_each(x, axis):
    count = lax.axis_size(axis)
    return lax.all_to_all(jnp.broadcast_to(x[None], (count, *x.shape)), axis, 0, 0, tiled=True)


def over_copies(x, axis):
    everything = copy_for_each(x, axis)
    return jnp.sum(everything, axis=0)


def laid_out(tiles, dim):
    dims = list(tiles.shape[1:])
    dims[dim] *= tiles.shape[0]
    return jnp.moveaxis(tiles, 0, dim).reshape(dims)


def collect(x, axis, dim):
    tiles = copy_for_each(x, axis)
    return laid_out(tiles, dim)


def in_one(arrays, axis):
    ends = [0]
    for a in arrays:
        ends.append(ends[-1] + a.size)
    so_far = over_copies(jnp.concatenate([a.ravel() for a in arrays]), axis)
    return tuple((so_far[b:e].reshape(a.shape) for a, b, e in zip(arrays, ends, ends[1:])))


def histogram(bucket, label, group, group_weight, start, count):
    choose = group[:, None] == jnp.arange(group_weight.shape[0])[None, :]
    weight = jnp.sum(jnp.where(choose, group_weight[None, :], 0.0), axis=1)
    labels = label.astype(jnp.float32)
    positive = (weight * labels).astype(jnp.bfloat16)
    negative = (weight * (1.0 - labels)).astype(jnp.bfloat16)
    rows = bucket.shape[0]
    width = BLOCK
    blocks = rows // width

    def accumulate(total, items):
        ids, plus, minus = items
        high = ids // LO
        low = ids % LO
        high_one = high[:, None] == start + jnp.arange(count)[None, :]
        zero = jnp.zeros((), jnp.bfloat16)
        left = jnp.stack(
            [jnp.where(high_one, plus[:, None], zero), jnp.where(high_one, minus[:, None], zero)],
            axis=2,
        )
        left = left.reshape(width, count * 2)
        low_one = (low[:, None] == jnp.arange(LO)[None, :]).astype(jnp.bfloat16)
        product = lax.dot_general(
            left, low_one, (((0,), (0,)), ((), ())), preferred_element_type=jnp.float32
        )
        return (total + product, None)

    initial = jnp.zeros((count * 2, LO), jnp.float32)
    items = (
        bucket.reshape(blocks, width),
        positive.reshape(blocks, width),
        negative.reshape(blocks, width),
    )
    total, _ = lax.scan(accumulate, initial, items)
    return total.reshape(count, 2, LO)


def general(bucket, label, group, group_weight):
    shards = lax.axis_size("shard")
    own_rows = HI // shards
    first_row = lax.axis_index("shard") * own_rows
    ids = lax.all_gather(bucket, "shard", axis=0, tiled=True)
    clicks = lax.all_gather(label, "shard", axis=0, tiled=True)
    groups = lax.all_gather(group, "shard", axis=0, tiled=True)
    owned = histogram(ids, clicks, groups, group_weight, first_row, own_rows)
    owned = over_copies(owned, "grp")
    upper = (jnp.arange(LO)[:, None] >= jnp.arange(LO)[None, :]).astype(jnp.float32)
    row_suffix = jnp.dot(owned.reshape(own_rows * 2, LO), upper, precision=HIGHEST)
    row_totals = jnp.sum(owned, axis=2)
    strict = (jnp.arange(own_rows)[None, :] > jnp.arange(own_rows)[:, None]).astype(jnp.float32)
    after = jnp.dot(strict, row_totals, precision=HIGHEST)
    range_total = jnp.sum(row_totals, axis=0)
    every = collect(range_total[None, :], "shard", 0)
    later = jnp.arange(shards) > lax.axis_index("shard")
    higher = jnp.sum(jnp.where(later[:, None], every, 0.0), axis=0)
    overall = jnp.sum(every, axis=0)
    cumulative = row_suffix.reshape(own_rows, 2, LO) + after[:, :, None] + higher[None, :, None]
    true_pos = cumulative[:, 0, :]
    false_pos = cumulative[:, 1, :]
    pos_hist = owned[:, 0, :]
    neg_hist = owned[:, 1, :]
    tpr_curve = (true_pos / overall[0]).reshape(own_rows * LO)
    precision = true_pos / jnp.maximum(true_pos + false_pos, 1.0)
    roc_part = jnp.sum(neg_hist * (2.0 * true_pos - pos_hist))
    prc_part = jnp.sum(pos_hist * precision)
    roc_sum, prc_sum = in_one((roc_part, prc_part), "shard")
    auroc = roc_sum / (2.0 * overall[0] * overall[1])
    auprc = prc_sum / overall[0]
    return (tpr_curve, precision.reshape(own_rows * LO), auroc, auprc)


def iota(shape, dim):
    return lax.broadcasted_iota(jnp.int32, shape, dim)


def bf16_rows(row):
    return jnp.broadcast_to(row, (16, row.shape[1])).astype(jnp.bfloat16)


def route_kernel(weights_ref, bucket_ref, label_ref, group_ref, out_ref,
                 peer_s, high_s, low_s, pos_s, neg_s, one_s, left_s, right_s, acc_s):
    blocks = bucket_ref.shape[0]
    step = 8
    bucket = bucket_ref[...]
    group = group_ref[...]
    weight = jnp.zeros(group.shape, jnp.float32)
    for k in range(weights_ref.shape[0]):
        weight = jnp.where(group == k, weights_ref[k], weight)
    labels = label_ref[...].astype(jnp.float32)
    pos_s[...] = weight * labels
    neg_s[...] = weight * (1.0 - labels)
    which = bucket >> RANGE_BITS
    peer = ((which & 3) << 5) | (which >> 2)
    peer_s[...] = peer.astype(jnp.float32)
    high_s[...] = ((bucket >> 7) & (ROWS - 1)).astype(jnp.float32)
    low_s[...] = (bucket & (LANES - 1)).astype(jnp.float32)

    before = (iota((LANES, 2 * LANES), 0) < iota((LANES, 2 * LANES), 1)).astype(jnp.bfloat16)
    sub = iota((16, LANES), 0)
    unit = jnp.ones((16, LANES), jnp.bfloat16)
    none = jnp.zeros((16, LANES), jnp.bfloat16)
    kind = sub & 3
    sub_f = sub.astype(jnp.float32).astype(jnp.bfloat16)
    quarter_f = (sub >> 2).astype(jnp.float32).astype(jnp.bfloat16)
    acc_s[...] = jnp.zeros(acc_s.shape, jnp.float32)

    def chunk(i, count):
        for u in range(step):
            row = bf16_rows(peer_s[pl.ds(i * step + u, 1), :])
            for k in range(8):
                one_s[pl.ds(u * LANES + 16 * k, 16), :] = jnp.where(
                    sub_f + jnp.bfloat16(16 * k) == row, unit, none)
        ones = one_s[...]
        seen = lax.dot_general(ones, before, NN, preferred_element_type=jnp.float32)
        for u in range(step):
            mine = ones[u * LANES:(u + 1) * LANES].astype(jnp.float32)
            part = seen[u * LANES:(u + 1) * LANES]
            rank = jnp.sum(mine * (part[:, :LANES] + count), axis=0, keepdims=True)
            count = count + part[:, LANES:]
            j = i * step + u
            lanes = pl.ds(u * LANES, LANES)
            rank_row = bf16_rows(jnp.minimum(rank, 255.0))
            for k in range(8):
                right_s[pl.ds(16 * k, 16), lanes] = jnp.where(
                    sub_f + jnp.bfloat16(16 * k) == rank_row, unit, none)
            high = jnp.broadcast_to(high_s[pl.ds(j, 1), :], (16, LANES))
            low = jnp.broadcast_to(low_s[pl.ds(j, 1), :], (16, LANES))
            pos = jnp.broadcast_to(pos_s[pl.ds(j, 1), :], (16, LANES))
            neg = jnp.broadcast_to(neg_s[pl.ds(j, 1), :], (16, LANES))
            value = jnp.where(kind == 0, high, jnp.where(kind == 1, low, jnp.where(kind == 2, pos, neg)))
            value = value.astype(jnp.bfloat16)
            row = bf16_rows(peer_s[pl.ds(j, 1), :])
            for k in range(32):
                left_s[pl.ds(16 * k, 16), lanes] = jnp.where(
                    quarter_f + jnp.bfloat16(4 * k) == row, value, none)
        acc_s[...] += lax.dot_general(left_s[...], right_s[...], NT, preferred_element_type=jnp.float32)
        return count

    count = lax.fori_loop(0, blocks // step, chunk, jnp.zeros((RANGES, LANES), jnp.float32))
    full = jnp.max(jnp.where(count > CAP, 1.0, 0.0), axis=0, keepdims=True)
    full = jnp.max(full, axis=1, keepdims=True)

    lane = iota((RANGES, LANES), 1)
    real = lane < CAP
    high = acc_s[pl.ds(0, RANGES, stride=4), :]
    low = acc_s[pl.ds(1, RANGES, stride=4), :]
    pos = jnp.where(real, acc_s[pl.ds(2, RANGES, stride=4), :], 0.0)
    neg = jnp.where(real, acc_s[pl.ds(3, RANGES, stride=4), :], 0.0)
    p0 = iota((RANGES, RANGES), 0)
    p1 = iota((RANGES, RANGES), 1)
    r0 = ((p0 & 31) << 2) | (p0 >> 5)
    r1 = ((p1 & 31) << 2) | (p1 >> 5)
    above = (r1 > r0).astype(jnp.bfloat16)
    both = jnp.concatenate([pos, neg], axis=1).astype(jnp.bfloat16)
    later = lax.dot_general(above, both, NN, preferred_element_type=jnp.float32)
    higher_pos = jnp.sum(later[:, :LANES], axis=1, keepdims=True)
    higher_neg = jnp.sum(later[:, LANES:], axis=1, keepdims=True)
    total_pos = jnp.sum(jnp.sum(pos, axis=0, keepdims=True), axis=1, keepdims=True)
    total_neg = jnp.sum(jnp.sum(neg, axis=0, keepdims=True), axis=1, keepdims=True)
    out_ref[pl.ds(0, RANGES, stride=4), :] = jnp.where(real, high, full)
    out_ref[pl.ds(1, RANGES, stride=4), :] = low
    out_ref[pl.ds(2, RANGES, stride=4), :] = jnp.where(real, pos, jnp.where(lane == CAP, higher_pos, total_pos))
    out_ref[pl.ds(3, RANGES, stride=4), :] = jnp.where(real, neg, jnp.where(lane == CAP, higher_neg, total_neg))


def curve_kernel(in_ref, curve_ref, part_ref, left_s, right_s):
    step = 8
    sub_f = iota((16, LANES), 0).astype(jnp.float32).astype(jnp.bfloat16)
    none = jnp.zeros((16, LANES), jnp.bfloat16)
    unit = jnp.ones((16, LANES), jnp.bfloat16)
    real = iota((1, LANES), 1) < CAP

    def chunk(i, carry):
        hist, sums = carry
        for u in range(step):
            at = (i * step + u) * 4
            lanes = pl.ds(u * LANES, LANES)
            high = bf16_rows(in_ref[pl.ds(at, 1), :])
            low = bf16_rows(in_ref[pl.ds(at + 1, 1), :])
            pos = bf16_rows(jnp.where(real, in_ref[pl.ds(at + 2, 1), :], 0.0))
            neg = bf16_rows(jnp.where(real, in_ref[pl.ds(at + 3, 1), :], 0.0))
            for k in range(4):
                same = sub_f + jnp.bfloat16(16 * k) == high
                left_s[pl.ds(16 * k, 16), lanes] = jnp.where(same, pos, none)
                left_s[pl.ds(ROWS + 16 * k, 16), lanes] = jnp.where(same, neg, none)
            for k in range(8):
                right_s[pl.ds(16 * k, 16), lanes] = jnp.where(
                    sub_f + jnp.bfloat16(16 * k) == low, unit, none)
        hist = hist + lax.dot_general(left_s[...], right_s[...], NT, preferred_element_type=jnp.float32)
        for u in range(step // 2):
            sums = sums + in_ref[pl.ds((i * step + 2 * u) * 4, 8), :]
        return hist, sums

    start = (jnp.zeros((2 * ROWS, LANES), jnp.float32), jnp.zeros((8, LANES), jnp.float32))
    hist, sums = lax.fori_loop(0, RANGES // step, chunk, start)
    sums = sums[0:4] + sums[4:8]
    flag = sums[0:1, CAP:CAP + 1]
    higher_pos = sums[2:3, CAP:CAP + 1]
    total_pos = sums[2:3, CAP + 1:CAP + 2]
    higher_neg = sums[3:4, CAP:CAP + 1]
    total_neg = sums[3:4, CAP + 1:CAP + 2]
    upper = (iota((LANES, LANES), 0) >= iota((LANES, LANES), 1)).astype(jnp.float32)
    row = iota((2 * ROWS, 2 * ROWS), 0)
    col = iota((2 * ROWS, 2 * ROWS), 1)
    below = ((col > row) & ((col >= ROWS) == (row >= ROWS))).astype(jnp.float32)
    in_row = lax.dot_general(hist, upper, NN, precision=HIGHEST, preferred_element_type=jnp.float32)
    rows_after = lax.dot_general(below, hist, NN, precision=HIGHEST, preferred_element_type=jnp.float32)
    cumulative = in_row + jnp.sum(rows_after, axis=1, keepdims=True)
    true_pos = cumulative[:ROWS] + higher_pos
    false_pos = cumulative[ROWS:] + higher_neg
    pos_hist = hist[:ROWS]
    neg_hist = hist[ROWS:]
    precision = true_pos / jnp.maximum(true_pos + false_pos, 1.0)
    curve_ref[0] = true_pos / total_pos
    curve_ref[1] = precision
    roc = jnp.sum(neg_hist * (2.0 * true_pos - pos_hist), axis=0, keepdims=True)
    prc = jnp.sum(pos_hist * precision, axis=0, keepdims=True)
    roc = jnp.sum(roc, axis=1, keepdims=True) / (2.0 * total_pos * total_neg)
    prc = jnp.sum(prc, axis=1, keepdims=True) / total_pos
    lane = iota((RANGES, 1, LANES), 2)
    part_ref[...] = jnp.where(lane == 0, roc[None], jnp.where(lane == 1, prc[None], flag[None]))


def join_kernel(own_ref, one_ref, two_ref, three_ref, part_ref, tpr_ref, precision_ref, roc_ref, prc_ref, flag_ref):
    me = lax.axis_index("grp")
    for k, ref in enumerate((own_ref, one_ref, two_ref, three_ref)):
        source = (me - k) & 3
        tpr_ref[source] = ref[0]
        precision_ref[source] = ref[1]
    sums = jnp.sum(part_ref[...].reshape(RANGES, LANES), axis=0, keepdims=True)
    lane = iota((1, LANES), 1)
    roc_ref[0] = jnp.sum(jnp.where(lane == 0, sums, 0.0))
    prc_ref[0] = jnp.sum(jnp.where(lane == 1, sums, 0.0))
    flag_ref[0] = jnp.sum(jnp.where(lane == 2, sums, 0.0))


def vmem():
    return pl.BlockSpec(memory_space=pltpu.VMEM)


def smem():
    return pl.BlockSpec(memory_space=pltpu.SMEM)


def f32(*shape):
    return jax.ShapeDtypeStruct(shape, jnp.float32)


def on_device(bucket, label, group, group_weight):
    blocks = bucket.shape[0] // LANES
    message = pl.pallas_call(
        route_kernel,
        out_shape=f32(4 * RANGES, LANES),
        in_specs=[smem(), vmem(), vmem(), vmem()],
        out_specs=vmem(),
        scratch_shapes=[pltpu.VMEM((blocks, LANES), jnp.float32)] * 5
        + [pltpu.VMEM((8 * LANES, LANES), jnp.bfloat16),
           pltpu.VMEM((4 * RANGES, 8 * LANES), jnp.bfloat16),
           pltpu.VMEM((LANES, 8 * LANES), jnp.bfloat16),
           pltpu.VMEM((4 * RANGES, LANES), jnp.float32)],
        name="route",
    )(group_weight, bucket.reshape(blocks, LANES), label.reshape(blocks, LANES), group.reshape(blocks, LANES))
    received = lax.all_to_all(message.reshape(RANGES, 4, LANES), AXES, 0, 0, tiled=True)
    curves, parts = pl.pallas_call(
        curve_kernel,
        out_shape=(f32(2, ROWS, LANES), f32(RANGES, 1, LANES)),
        in_specs=[vmem()],
        out_specs=(vmem(), vmem()),
        scratch_shapes=[pltpu.VMEM((2 * ROWS, 8 * LANES), jnp.bfloat16), pltpu.VMEM((LANES, 8 * LANES), jnp.bfloat16)],
        name="curve",
    )(received.reshape(4 * RANGES, LANES))
    others = [lax.ppermute(curves, "grp", [(i, (i + k) % 4) for i in range(4)]) for k in (1, 2, 3)]
    parts = lax.all_to_all(parts, AXES, 0, 0, tiled=True)
    tpr, precision, roc, prc, flag = pl.pallas_call(
        join_kernel,
        out_shape=(f32(4, ROWS, LANES), f32(4, ROWS, LANES), f32(1), f32(1), f32(1)),
        in_specs=[vmem()] * 5,
        out_specs=(vmem(), vmem(), smem(), smem(), smem()),
        name="join",
    )(curves, *others, parts)
    quick = (tpr.reshape(4 * ROWS * LANES), precision.reshape(4 * ROWS * LANES), roc.reshape(()), prc.reshape(()))

    def again(state):
        return (jnp.zeros((), jnp.float32), *general(bucket, label, group, group_weight))

    state = lax.while_loop(lambda s: s[0] > 0.0, again, (flag.reshape(()), *quick))
    return state[1:]


def solution(mesh):
    placed = (P(AXES), P(AXES), P(AXES), P())
    return jax.shard_map(
        on_device,
        mesh=mesh,
        in_specs=placed,
        out_specs=(P("shard"), P("shard"), P(), P()),
        check_vma=False,
    )
```

```python
import jax
import jax.numpy as jnp
from jax import lax
from jax.experimental import pallas as pl
from jax.experimental.pallas import tpu as pltpu
from jax.sharding import PartitionSpec as P


LO = 256
BLOCK = 1024
HI = 4096

AXES = ("grp", "shard")
LANES = 128
RANGES = 128
RANGE_BITS = 13
ROWS = 64
CAP = 126
NT = (((1,), (1,)), ((), ()))
NN = (((1,), (0,)), ((), ()))
HIGHEST = lax.Precision.HIGHEST


def copy_for_each(x, axis):
    count = lax.axis_size(axis)
    return lax.all_to_all(jnp.broadcast_to(x[None], (count, *x.shape)), axis, 0, 0, tiled=True)


def over_copies(x, axis):
    everything = copy_for_each(x, axis)
    return jnp.sum(everything, axis=0)


def laid_out(tiles, dim):
    dims = list(tiles.shape[1:])
    dims[dim] *= tiles.shape[0]
    return jnp.moveaxis(tiles, 0, dim).reshape(dims)


def collect(x, axis, dim):
    tiles = copy_for_each(x, axis)
    return laid_out(tiles, dim)


def in_one(arrays, axis):
    ends = [0]
    for a in arrays:
        ends.append(ends[-1] + a.size)
    so_far = over_copies(jnp.concatenate([a.ravel() for a in arrays]), axis)
    return tuple((so_far[b:e].reshape(a.shape) for a, b, e in zip(arrays, ends, ends[1:])))


def histogram(bucket, label, group, group_weight, start, count):
    choose = group[:, None] == jnp.arange(group_weight.shape[0])[None, :]
    weight = jnp.sum(jnp.where(choose, group_weight[None, :], 0.0), axis=1)
    labels = label.astype(jnp.float32)
    positive = (weight * labels).astype(jnp.bfloat16)
    negative = (weight * (1.0 - labels)).astype(jnp.bfloat16)
    rows = bucket.shape[0]
    width = BLOCK
    blocks = rows // width

    def accumulate(total, items):
        ids, plus, minus = items
        high = ids // LO
        low = ids % LO
        high_one = high[:, None] == start + jnp.arange(count)[None, :]
        zero = jnp.zeros((), jnp.bfloat16)
        left = jnp.stack(
            [jnp.where(high_one, plus[:, None], zero), jnp.where(high_one, minus[:, None], zero)],
            axis=2,
        )
        left = left.reshape(width, count * 2)
        low_one = (low[:, None] == jnp.arange(LO)[None, :]).astype(jnp.bfloat16)
        product = lax.dot_general(
            left, low_one, (((0,), (0,)), ((), ())), preferred_element_type=jnp.float32
        )
        return (total + product, None)

    initial = jnp.zeros((count * 2, LO), jnp.float32)
    items = (
        bucket.reshape(blocks, width),
        positive.reshape(blocks, width),
        negative.reshape(blocks, width),
    )
    total, _ = lax.scan(accumulate, initial, items)
    return total.reshape(count, 2, LO)


def general(bucket, label, group, group_weight):
    shards = lax.axis_size("shard")
    own_rows = HI // shards
    first_row = lax.axis_index("shard") * own_rows
    ids = lax.all_gather(bucket, "shard", axis=0, tiled=True)
    clicks = lax.all_gather(label, "shard", axis=0, tiled=True)
    groups = lax.all_gather(group, "shard", axis=0, tiled=True)
    owned = histogram(ids, clicks, groups, group_weight, first_row, own_rows)
    owned = over_copies(owned, "grp")
    upper = (jnp.arange(LO)[:, None] >= jnp.arange(LO)[None, :]).astype(jnp.float32)
    row_suffix = jnp.dot(owned.reshape(own_rows * 2, LO), upper, precision=HIGHEST)
    row_totals = jnp.sum(owned, axis=2)
    strict = (jnp.arange(own_rows)[None, :] > jnp.arange(own_rows)[:, None]).astype(jnp.float32)
    after = jnp.dot(strict, row_totals, precision=HIGHEST)
    range_total = jnp.sum(row_totals, axis=0)
    every = collect(range_total[None, :], "shard", 0)
    later = jnp.arange(shards) > lax.axis_index("shard")
    higher = jnp.sum(jnp.where(later[:, None], every, 0.0), axis=0)
    overall = jnp.sum(every, axis=0)
    cumulative = row_suffix.reshape(own_rows, 2, LO) + after[:, :, None] + higher[None, :, None]
    true_pos = cumulative[:, 0, :]
    false_pos = cumulative[:, 1, :]
    pos_hist = owned[:, 0, :]
    neg_hist = owned[:, 1, :]
    tpr_curve = (true_pos / overall[0]).reshape(own_rows * LO)
    precision = true_pos / jnp.maximum(true_pos + false_pos, 1.0)
    roc_part = jnp.sum(neg_hist * (2.0 * true_pos - pos_hist))
    prc_part = jnp.sum(pos_hist * precision)
    roc_sum, prc_sum = in_one((roc_part, prc_part), "shard")
    auroc = roc_sum / (2.0 * overall[0] * overall[1])
    auprc = prc_sum / overall[0]
    return (tpr_curve, precision.reshape(own_rows * LO), auroc, auprc)


def iota(shape, dim):
    return lax.broadcasted_iota(jnp.int32, shape, dim)


def bf16_rows(row):
    return jnp.broadcast_to(row, (16, row.shape[1])).astype(jnp.bfloat16)


def route_kernel(weights_ref, bucket_ref, label_ref, group_ref, out_ref,
                 peer_s, high_s, low_s, pos_s, neg_s, one_s, left_s, right_s, acc_s):
    blocks = bucket_ref.shape[0]
    step = 8
    bucket = bucket_ref[...]
    group = group_ref[...]
    weight = jnp.zeros(group.shape, jnp.float32)
    for k in range(weights_ref.shape[0]):
        weight = jnp.where(group == k, weights_ref[k], weight)
    labels = label_ref[...].astype(jnp.float32)
    pos_s[...] = weight * labels
    neg_s[...] = weight * (1.0 - labels)
    which = bucket >> RANGE_BITS
    peer = ((which & 3) << 5) | (which >> 2)
    peer_s[...] = peer.astype(jnp.float32)
    high_s[...] = ((bucket >> 7) & (ROWS - 1)).astype(jnp.float32)
    low_s[...] = (bucket & (LANES - 1)).astype(jnp.float32)

    before = (iota((LANES, 2 * LANES), 0) < iota((LANES, 2 * LANES), 1)).astype(jnp.bfloat16)
    sub = iota((16, LANES), 0)
    unit = jnp.ones((16, LANES), jnp.bfloat16)
    none = jnp.zeros((16, LANES), jnp.bfloat16)
    kind = sub & 3
    sub_f = sub.astype(jnp.float32).astype(jnp.bfloat16)
    quarter_f = (sub >> 2).astype(jnp.float32).astype(jnp.bfloat16)
    acc_s[...] = jnp.zeros(acc_s.shape, jnp.float32)

    def chunk(i, count):
        for u in range(step):
            row = bf16_rows(peer_s[pl.ds(i * step + u, 1), :])
            for k in range(8):
                one_s[pl.ds(u * LANES + 16 * k, 16), :] = jnp.where(
                    sub_f + jnp.bfloat16(16 * k) == row, unit, none)
        ones = one_s[...]
        seen = lax.dot_general(ones, before, NN, preferred_element_type=jnp.float32)
        for u in range(step):
            mine = ones[u * LANES:(u + 1) * LANES].astype(jnp.float32)
            part = seen[u * LANES:(u + 1) * LANES]
            rank = jnp.sum(mine * (part[:, :LANES] + count), axis=0, keepdims=True)
            count = count + part[:, LANES:]
            j = i * step + u
            lanes = pl.ds(u * LANES, LANES)
            rank_row = bf16_rows(jnp.minimum(rank, 255.0))
            for k in range(8):
                right_s[pl.ds(16 * k, 16), lanes] = jnp.where(
                    sub_f + jnp.bfloat16(16 * k) == rank_row, unit, none)
            high = jnp.broadcast_to(high_s[pl.ds(j, 1), :], (16, LANES))
            low = jnp.broadcast_to(low_s[pl.ds(j, 1), :], (16, LANES))
            pos = jnp.broadcast_to(pos_s[pl.ds(j, 1), :], (16, LANES))
            neg = jnp.broadcast_to(neg_s[pl.ds(j, 1), :], (16, LANES))
            value = jnp.where(kind == 0, high, jnp.where(kind == 1, low, jnp.where(kind == 2, pos, neg)))
            value = value.astype(jnp.bfloat16)
            row = bf16_rows(peer_s[pl.ds(j, 1), :])
            for k in range(32):
                left_s[pl.ds(16 * k, 16), lanes] = jnp.where(
                    quarter_f + jnp.bfloat16(4 * k) == row, value, none)
        acc_s[...] += lax.dot_general(left_s[...], right_s[...], NT, preferred_element_type=jnp.float32)
        return count

    count = lax.fori_loop(0, blocks // step, chunk, jnp.zeros((RANGES, LANES), jnp.float32))
    full = jnp.max(jnp.where(count > CAP, 1.0, 0.0), axis=0, keepdims=True)
    full = jnp.max(full, axis=1, keepdims=True)

    lane = iota((RANGES, LANES), 1)
    real = lane < CAP
    high = acc_s[pl.ds(0, RANGES, stride=4), :]
    low = acc_s[pl.ds(1, RANGES, stride=4), :]
    pos = jnp.where(real, acc_s[pl.ds(2, RANGES, stride=4), :], 0.0)
    neg = jnp.where(real, acc_s[pl.ds(3, RANGES, stride=4), :], 0.0)
    p0 = iota((RANGES, RANGES), 0)
    p1 = iota((RANGES, RANGES), 1)
    r0 = ((p0 & 31) << 2) | (p0 >> 5)
    r1 = ((p1 & 31) << 2) | (p1 >> 5)
    above = (r1 > r0).astype(jnp.bfloat16)
    both = jnp.concatenate([pos, neg], axis=1).astype(jnp.bfloat16)
    later = lax.dot_general(above, both, NN, preferred_element_type=jnp.float32)
    higher_pos = jnp.sum(later[:, :LANES], axis=1, keepdims=True)
    higher_neg = jnp.sum(later[:, LANES:], axis=1, keepdims=True)
    total_pos = jnp.sum(jnp.sum(pos, axis=0, keepdims=True), axis=1, keepdims=True)
    total_neg = jnp.sum(jnp.sum(neg, axis=0, keepdims=True), axis=1, keepdims=True)
    out_ref[pl.ds(0, RANGES, stride=4), :] = jnp.where(real, high, full)
    out_ref[pl.ds(1, RANGES, stride=4), :] = low
    out_ref[pl.ds(2, RANGES, stride=4), :] = jnp.where(real, pos, jnp.where(lane == CAP, higher_pos, total_pos))
    out_ref[pl.ds(3, RANGES, stride=4), :] = jnp.where(real, neg, jnp.where(lane == CAP, higher_neg, total_neg))


def curve_kernel(in_ref, curve_ref, part_ref, left_s, right_s):
    step = 8
    sub_f = iota((16, LANES), 0).astype(jnp.float32).astype(jnp.bfloat16)
    none = jnp.zeros((16, LANES), jnp.bfloat16)
    unit = jnp.ones((16, LANES), jnp.bfloat16)
    real = iota((1, LANES), 1) < CAP

    def chunk(i, carry):
        hist, sums = carry
        for u in range(step):
            at = (i * step + u) * 4
            lanes = pl.ds(u * LANES, LANES)
            high = bf16_rows(in_ref[pl.ds(at, 1), :])
            low = bf16_rows(in_ref[pl.ds(at + 1, 1), :])
            pos = bf16_rows(jnp.where(real, in_ref[pl.ds(at + 2, 1), :], 0.0))
            neg = bf16_rows(jnp.where(real, in_ref[pl.ds(at + 3, 1), :], 0.0))
            for k in range(4):
                same = sub_f + jnp.bfloat16(16 * k) == high
                left_s[pl.ds(16 * k, 16), lanes] = jnp.where(same, pos, none)
                left_s[pl.ds(ROWS + 16 * k, 16), lanes] = jnp.where(same, neg, none)
            for k in range(8):
                right_s[pl.ds(16 * k, 16), lanes] = jnp.where(
                    sub_f + jnp.bfloat16(16 * k) == low, unit, none)
        hist = hist + lax.dot_general(left_s[...], right_s[...], NT, preferred_element_type=jnp.float32)
        for u in range(step // 2):
            sums = sums + in_ref[pl.ds((i * step + 2 * u) * 4, 8), :]
        return hist, sums

    start = (jnp.zeros((2 * ROWS, LANES), jnp.float32), jnp.zeros((8, LANES), jnp.float32))
    hist, sums = lax.fori_loop(0, RANGES // step, chunk, start)
    sums = sums[0:4] + sums[4:8]
    flag = sums[0:1, CAP:CAP + 1]
    higher_pos = sums[2:3, CAP:CAP + 1]
    total_pos = sums[2:3, CAP + 1:CAP + 2]
    higher_neg = sums[3:4, CAP:CAP + 1]
    total_neg = sums[3:4, CAP + 1:CAP + 2]
    upper = (iota((LANES, LANES), 0) >= iota((LANES, LANES), 1)).astype(jnp.float32)
    row = iota((2 * ROWS, 2 * ROWS), 0)
    col = iota((2 * ROWS, 2 * ROWS), 1)
    below = ((col > row) & ((col >= ROWS) == (row >= ROWS))).astype(jnp.float32)
    in_row = lax.dot_general(hist, upper, NN, precision=HIGHEST, preferred_element_type=jnp.float32)
    rows_after = lax.dot_general(below, hist, NN, precision=HIGHEST, preferred_element_type=jnp.float32)
    cumulative = in_row + jnp.sum(rows_after, axis=1, keepdims=True)
    true_pos = cumulative[:ROWS] + higher_pos
    false_pos = cumulative[ROWS:] + higher_neg
    pos_hist = hist[:ROWS]
    neg_hist = hist[ROWS:]
    precision = true_pos / jnp.maximum(true_pos + false_pos, 1.0)
    curve_ref[0] = true_pos / total_pos
    curve_ref[1] = precision
    roc = jnp.sum(neg_hist * (2.0 * true_pos - pos_hist), axis=0, keepdims=True)
    prc = jnp.sum(pos_hist * precision, axis=0, keepdims=True)
    roc = jnp.sum(roc, axis=1, keepdims=True) / (2.0 * total_pos * total_neg)
    prc = jnp.sum(prc, axis=1, keepdims=True) / total_pos
    lane = iota((RANGES, 1, LANES), 2)
    part_ref[...] = jnp.where(lane == 0, roc[None], jnp.where(lane == 1, prc[None], flag[None]))


def join_kernel(own_ref, one_ref, two_ref, three_ref, tpr_ref, precision_ref):
    me = lax.axis_index("grp")
    for k, ref in enumerate((own_ref, one_ref, two_ref, three_ref)):
        source = (me - k) & 3
        tpr_ref[source] = ref[0]
        precision_ref[source] = ref[1]


def area_kernel(part_ref, roc_ref, prc_ref, flag_ref):
    sums = jnp.sum(part_ref[...].reshape(RANGES, LANES), axis=0, keepdims=True)
    lane = iota((1, LANES), 1)
    roc_ref[0] = jnp.sum(jnp.where(lane == 0, sums, 0.0))
    prc_ref[0] = jnp.sum(jnp.where(lane == 1, sums, 0.0))
    flag_ref[0] = jnp.sum(jnp.where(lane == 2, sums, 0.0))


def vmem():
    return pl.BlockSpec(memory_space=pltpu.VMEM)


def smem():
    return pl.BlockSpec(memory_space=pltpu.SMEM)


def f32(*shape):
    return jax.ShapeDtypeStruct(shape, jnp.float32)


def near(*shape):
    return pltpu.VMEM(shape, jnp.float32)


def at_hand(x):
    return pltpu.with_memory_space_constraint(x, pltpu.VMEM)


def on_device(bucket, label, group, group_weight):
    blocks = bucket.shape[0] // LANES
    message = pl.pallas_call(
        route_kernel,
        out_shape=near(4 * RANGES, LANES),
        in_specs=[smem(), vmem(), vmem(), vmem()],
        out_specs=vmem(),
        scratch_shapes=[pltpu.VMEM((blocks, LANES), jnp.float32)] * 5
        + [pltpu.VMEM((8 * LANES, LANES), jnp.bfloat16),
           pltpu.VMEM((4 * RANGES, 8 * LANES), jnp.bfloat16),
           pltpu.VMEM((LANES, 8 * LANES), jnp.bfloat16),
           pltpu.VMEM((4 * RANGES, LANES), jnp.float32)],
        name="route",
    )(group_weight, bucket.reshape(blocks, LANES), label.reshape(blocks, LANES), group.reshape(blocks, LANES))
    received = lax.all_to_all(message.reshape(RANGES, 4, LANES), AXES, 0, 0, tiled=True)
    curves, parts = pl.pallas_call(
        curve_kernel,
        out_shape=(near(2, ROWS, LANES), near(RANGES, 1, LANES)),
        in_specs=[vmem()],
        out_specs=(vmem(), vmem()),
        scratch_shapes=[pltpu.VMEM((2 * ROWS, 8 * LANES), jnp.bfloat16), pltpu.VMEM((LANES, 8 * LANES), jnp.bfloat16)],
        name="curve",
    )(at_hand(received.reshape(4 * RANGES, LANES)))
    parts = lax.all_to_all(parts, AXES, 0, 0, tiled=True)
    others = [lax.ppermute(curves, "grp", [(i, (i + k) % 4) for i in range(4)]) for k in (1, 2, 3)]
    tpr, precision = pl.pallas_call(
        join_kernel,
        out_shape=(f32(4, ROWS, LANES), f32(4, ROWS, LANES)),
        in_specs=[vmem()] * 4,
        out_specs=(vmem(), vmem()),
        name="join",
    )(at_hand(curves), *[at_hand(x) for x in others])
    roc, prc, flag = pl.pallas_call(
        area_kernel,
        out_shape=(f32(1), f32(1), f32(1)),
        in_specs=[vmem()],
        out_specs=(smem(), smem(), smem()),
        name="area",
    )(at_hand(parts))
    quick = (tpr.reshape(4 * ROWS * LANES), precision.reshape(4 * ROWS * LANES), roc.reshape(()), prc.reshape(()))

    def again(state):
        return (jnp.zeros((), jnp.float32), *general(bucket, label, group, group_weight))

    state = lax.while_loop(lambda s: s[0] > 0.0, again, (flag.reshape(()), *quick))
    return state[1:]


def solution(mesh):
    placed = (P(AXES), P(AXES), P(AXES), P())
    return jax.shard_map(
        on_device,
        mesh=mesh,
        in_specs=placed,
        out_specs=(P("shard"), P("shard"), P(), P()),
        check_vma=False,
    )
```

```python
import jax
import jax.numpy as jnp
from jax import lax
from jax.experimental import pallas as pl
from jax.experimental.pallas import tpu as pltpu
from jax.sharding import PartitionSpec as P


LO = 256
BLOCK = 1024
HI = 4096

AXES = ("grp", "shard")
LANES = 128
RANGES = 128
RANGE_BITS = 13
ROWS = 64
CAP = 126
NT = (((1,), (1,)), ((), ()))
NN = (((1,), (0,)), ((), ()))
HIGHEST = lax.Precision.HIGHEST


def copy_for_each(x, axis):
    count = lax.axis_size(axis)
    return lax.all_to_all(jnp.broadcast_to(x[None], (count, *x.shape)), axis, 0, 0, tiled=True)


def over_copies(x, axis):
    everything = copy_for_each(x, axis)
    return jnp.sum(everything, axis=0)


def laid_out(tiles, dim):
    dims = list(tiles.shape[1:])
    dims[dim] *= tiles.shape[0]
    return jnp.moveaxis(tiles, 0, dim).reshape(dims)


def collect(x, axis, dim):
    tiles = copy_for_each(x, axis)
    return laid_out(tiles, dim)


def in_one(arrays, axis):
    ends = [0]
    for a in arrays:
        ends.append(ends[-1] + a.size)
    so_far = over_copies(jnp.concatenate([a.ravel() for a in arrays]), axis)
    return tuple((so_far[b:e].reshape(a.shape) for a, b, e in zip(arrays, ends, ends[1:])))


def histogram(bucket, label, group, group_weight, start, count):
    choose = group[:, None] == jnp.arange(group_weight.shape[0])[None, :]
    weight = jnp.sum(jnp.where(choose, group_weight[None, :], 0.0), axis=1)
    labels = label.astype(jnp.float32)
    positive = (weight * labels).astype(jnp.bfloat16)
    negative = (weight * (1.0 - labels)).astype(jnp.bfloat16)
    rows = bucket.shape[0]
    width = BLOCK
    blocks = rows // width

    def accumulate(total, items):
        ids, plus, minus = items
        high = ids // LO
        low = ids % LO
        high_one = high[:, None] == start + jnp.arange(count)[None, :]
        zero = jnp.zeros((), jnp.bfloat16)
        left = jnp.stack(
            [jnp.where(high_one, plus[:, None], zero), jnp.where(high_one, minus[:, None], zero)],
            axis=2,
        )
        left = left.reshape(width, count * 2)
        low_one = (low[:, None] == jnp.arange(LO)[None, :]).astype(jnp.bfloat16)
        product = lax.dot_general(
            left, low_one, (((0,), (0,)), ((), ())), preferred_element_type=jnp.float32
        )
        return (total + product, None)

    initial = jnp.zeros((count * 2, LO), jnp.float32)
    items = (
        bucket.reshape(blocks, width),
        positive.reshape(blocks, width),
        negative.reshape(blocks, width),
    )
    total, _ = lax.scan(accumulate, initial, items)
    return total.reshape(count, 2, LO)


def general(bucket, label, group, group_weight):
    shards = lax.axis_size("shard")
    own_rows = HI // shards
    first_row = lax.axis_index("shard") * own_rows
    ids = lax.all_gather(bucket, "shard", axis=0, tiled=True)
    clicks = lax.all_gather(label, "shard", axis=0, tiled=True)
    groups = lax.all_gather(group, "shard", axis=0, tiled=True)
    owned = histogram(ids, clicks, groups, group_weight, first_row, own_rows)
    owned = over_copies(owned, "grp")
    upper = (jnp.arange(LO)[:, None] >= jnp.arange(LO)[None, :]).astype(jnp.float32)
    row_suffix = jnp.dot(owned.reshape(own_rows * 2, LO), upper, precision=HIGHEST)
    row_totals = jnp.sum(owned, axis=2)
    strict = (jnp.arange(own_rows)[None, :] > jnp.arange(own_rows)[:, None]).astype(jnp.float32)
    after = jnp.dot(strict, row_totals, precision=HIGHEST)
    range_total = jnp.sum(row_totals, axis=0)
    every = collect(range_total[None, :], "shard", 0)
    later = jnp.arange(shards) > lax.axis_index("shard")
    higher = jnp.sum(jnp.where(later[:, None], every, 0.0), axis=0)
    overall = jnp.sum(every, axis=0)
    cumulative = row_suffix.reshape(own_rows, 2, LO) + after[:, :, None] + higher[None, :, None]
    true_pos = cumulative[:, 0, :]
    false_pos = cumulative[:, 1, :]
    pos_hist = owned[:, 0, :]
    neg_hist = owned[:, 1, :]
    tpr_curve = (true_pos / overall[0]).reshape(own_rows * LO)
    precision = true_pos / jnp.maximum(true_pos + false_pos, 1.0)
    roc_part = jnp.sum(neg_hist * (2.0 * true_pos - pos_hist))
    prc_part = jnp.sum(pos_hist * precision)
    roc_sum, prc_sum = in_one((roc_part, prc_part), "shard")
    auroc = roc_sum / (2.0 * overall[0] * overall[1])
    auprc = prc_sum / overall[0]
    return (tpr_curve, precision.reshape(own_rows * LO), auroc, auprc)


def iota(shape, dim):
    return lax.broadcasted_iota(jnp.int32, shape, dim)


def bf16_rows(row):
    return jnp.broadcast_to(row, (16, row.shape[1])).astype(jnp.bfloat16)


def one_hot(row, groups, value, none):
    first = iota((16, LANES), 0).astype(jnp.float32).astype(jnp.bfloat16)
    return [jnp.where(first + jnp.bfloat16(16 * k) == row, value, none) for k in range(groups)]


def route_kernel(weights_ref, bucket_ref, label_ref, group_ref, out_ref,
                 peer_s, high_s, low_s, sign_s, part_s, acc_s):
    blocks = bucket_ref.shape[0]
    step = 48
    bucket = bucket_ref[...]
    group = group_ref[...]
    weight = jnp.zeros(group.shape, jnp.float32)
    for k in range(weights_ref.shape[0]):
        weight = jnp.where(group == k, weights_ref[k], weight)
    labels = label_ref[...].astype(jnp.float32)
    positive = (weight * labels).astype(jnp.bfloat16).astype(jnp.float32)
    negative = (weight * (1.0 - labels)).astype(jnp.bfloat16).astype(jnp.float32)
    sign_s[...] = positive - negative
    which = bucket >> RANGE_BITS
    peer = ((which & 3) << 5) | (which >> 2)
    peer_s[...] = peer.astype(jnp.float32)
    high_s[...] = ((bucket >> 7) & (ROWS - 1)).astype(jnp.float32)
    low_s[...] = (bucket & (LANES - 1)).astype(jnp.float32)

    wide = 2 * LANES
    upto = (iota((wide, wide), 0) <= iota((wide, wide), 1)).astype(jnp.bfloat16)
    none = jnp.zeros((16, LANES), jnp.bfloat16)
    unit = jnp.ones((16, LANES), jnp.bfloat16)
    acc_s[...] = jnp.zeros(acc_s.shape, jnp.float32)

    def chunk(i, count):
        ones = []
        for u in range(step):
            row = bf16_rows(peer_s[pl.ds(i * step + u, 1), :])
            ones.append(jnp.concatenate(one_hot(row, 8, unit, none), axis=0))
        for v in range(step // 2):
            pair = jnp.concatenate([ones[2 * v], ones[2 * v + 1]], axis=1)
            seen = lax.dot_general(pair, upto, NN, preferred_element_type=jnp.float32)
            for h in range(2):
                u = 2 * v + h
                mine = ones[u].astype(jnp.float32)
                before = seen[:, h * LANES:(h + 1) * LANES] + count
                rank = jnp.sum(mine * before, axis=0, keepdims=True) - 1.0
                rank = bf16_rows(jnp.minimum(rank, 255.0))
                j = i * step + u
                high = bf16_rows(high_s[pl.ds(j, 1), :])
                low = bf16_rows(low_s[pl.ds(j, 1), :])
                sign = bf16_rows(sign_s[pl.ds(j, 1), :])
                first = iota((16, LANES), 0).astype(jnp.float32).astype(jnp.bfloat16)
                for k in range(8):
                    same = first + jnp.bfloat16(16 * k) == rank
                    part_s[u, pl.ds(16 * k, 16), :] = jnp.where(same, high, none)
                    part_s[u, pl.ds(LANES + 16 * k, 16), :] = jnp.where(same, low, none)
                    part_s[u, pl.ds(2 * LANES + 16 * k, 16), :] = jnp.where(same, sign, none)
            count = count + jnp.broadcast_to(seen[:, wide - 1:wide], (RANGES, LANES))
        left = jnp.concatenate([part_s[u] for u in range(step)], axis=1)
        right = jnp.concatenate(ones, axis=1)
        acc_s[...] += lax.dot_general(left, right, NT, preferred_element_type=jnp.float32)
        return count

    count = lax.fori_loop(0, blocks // step, chunk, jnp.zeros((RANGES, LANES), jnp.float32))
    full = jnp.max(jnp.where(count > CAP, 1.0, 0.0), axis=0, keepdims=True)
    full = jnp.max(full, axis=1, keepdims=True)

    slot = iota((LANES, RANGES), 0)
    real = slot < CAP
    high = acc_s[pl.ds(0, LANES), :]
    low = acc_s[pl.ds(LANES, LANES), :]
    sign = jnp.where(real, acc_s[pl.ds(2 * LANES, LANES), :], 0.0)
    pos = jnp.maximum(sign, 0.0)
    neg = jnp.maximum(-sign, 0.0)
    p0 = iota((RANGES, RANGES), 0)
    p1 = iota((RANGES, RANGES), 1)
    r0 = ((p0 & 31) << 2) | (p0 >> 5)
    r1 = ((p1 & 31) << 2) | (p1 >> 5)
    above = (r0 > r1).astype(jnp.bfloat16)
    both = jnp.concatenate([pos, neg], axis=0).astype(jnp.bfloat16)
    later = lax.dot_general(both, above, NN, preferred_element_type=jnp.float32)
    for c, own in ((2, pos), (3, neg)):
        higher = jnp.sum(later[(c - 2) * LANES:(c - 1) * LANES], axis=0, keepdims=True)
        total = jnp.sum(jnp.sum(own, axis=0, keepdims=True), axis=1, keepdims=True)
        sent = jnp.where(real, own, jnp.where(slot == CAP, higher, total))
        out_ref[pl.ds(c, RANGES, stride=4), :] = sent.T
    out_ref[pl.ds(0, RANGES, stride=4), :] = jnp.where(real, high, full).T
    out_ref[pl.ds(1, RANGES, stride=4), :] = low.T


def in_three(x):
    first = x.astype(jnp.bfloat16)
    rest = x - first.astype(jnp.float32)
    second = rest.astype(jnp.bfloat16)
    rest = rest - second.astype(jnp.float32)
    return first, second, rest.astype(jnp.bfloat16)


def curve_kernel(in_ref, curve_ref, part_ref):
    step = 128
    none = jnp.zeros((16, LANES), jnp.bfloat16)
    unit = jnp.ones((16, LANES), jnp.bfloat16)
    first = iota((16, LANES), 0).astype(jnp.float32).astype(jnp.bfloat16)
    real = iota((16, LANES), 1) < CAP

    def chunk(i, carry):
        hist, sums = carry
        left = []
        right = []
        for u in range(step):
            at = (i * step + u) * 4
            high = bf16_rows(in_ref[pl.ds(at, 1), :])
            low = bf16_rows(in_ref[pl.ds(at + 1, 1), :])
            pos = jnp.where(real, jnp.broadcast_to(in_ref[pl.ds(at + 2, 1), :], (16, LANES)), 0.0).astype(jnp.bfloat16)
            neg = jnp.where(real, jnp.broadcast_to(in_ref[pl.ds(at + 3, 1), :], (16, LANES)), 0.0).astype(jnp.bfloat16)
            same = [first + jnp.bfloat16(16 * k) == high for k in range(4)]
            left.append(jnp.concatenate(
                [jnp.where(m, pos, none) for m in same] + [jnp.where(m, neg, none) for m in same], axis=0))
            right.append(jnp.concatenate(one_hot(low, 8, unit, none), axis=0))
        hist = hist + lax.dot_general(jnp.concatenate(left, axis=1), jnp.concatenate(right, axis=1), NT,
                                      preferred_element_type=jnp.float32)
        for u in range(step // 2):
            sums = sums + in_ref[pl.ds((i * step + 2 * u) * 4, 8), :]
        return hist, sums

    start = (jnp.zeros((2 * ROWS, LANES), jnp.float32), jnp.zeros((8, LANES), jnp.float32))
    hist, sums = lax.fori_loop(0, RANGES // step, chunk, start)
    sums = sums[0:4] + sums[4:8]
    flag = sums[0:1, CAP:CAP + 1]
    higher_pos = sums[2:3, CAP:CAP + 1]
    total_pos = sums[2:3, CAP + 1:CAP + 2]
    higher_neg = sums[3:4, CAP:CAP + 1]
    total_neg = sums[3:4, CAP + 1:CAP + 2]
    upper = (iota((LANES, LANES), 0) >= iota((LANES, LANES), 1)).astype(jnp.bfloat16)
    row = iota((2 * ROWS, 2 * ROWS), 0)
    col = iota((2 * ROWS, 2 * ROWS), 1)
    below = ((col > row) & ((col >= ROWS) == (row >= ROWS))).astype(jnp.bfloat16)
    pieces = in_three(hist)
    in_row = lax.dot_general(jnp.concatenate(pieces, axis=1), jnp.concatenate([upper] * 3, axis=0), NN,
                             preferred_element_type=jnp.float32)
    rows_after = lax.dot_general(jnp.concatenate([below] * 3, axis=1), jnp.concatenate(pieces, axis=0), NN,
                                 preferred_element_type=jnp.float32)
    cumulative = in_row + jnp.sum(rows_after, axis=1, keepdims=True)
    true_pos = cumulative[:ROWS] + higher_pos
    false_pos = cumulative[ROWS:] + higher_neg
    pos_hist = hist[:ROWS]
    neg_hist = hist[ROWS:]
    precision = true_pos / jnp.maximum(true_pos + false_pos, 1.0)
    curve_ref[0] = true_pos / total_pos
    curve_ref[1] = precision
    roc = jnp.sum(neg_hist * (2.0 * true_pos - pos_hist), axis=0, keepdims=True)
    prc = jnp.sum(pos_hist * precision, axis=0, keepdims=True)
    roc = jnp.sum(roc, axis=1, keepdims=True) / (2.0 * total_pos * total_neg)
    prc = jnp.sum(prc, axis=1, keepdims=True) / total_pos
    lane = iota((RANGES, 1, LANES), 2)
    part_ref[...] = jnp.where(lane == 0, roc[None], jnp.where(lane == 1, prc[None], flag[None]))


def join_kernel(own_ref, one_ref, two_ref, three_ref, tpr_ref, precision_ref):
    me = lax.axis_index("grp")
    for k, ref in enumerate((own_ref, one_ref, two_ref, three_ref)):
        source = (me - k) & 3
        tpr_ref[source] = ref[0]
        precision_ref[source] = ref[1]


def area_kernel(part_ref, roc_ref, prc_ref, flag_ref):
    sums = jnp.sum(part_ref[...].reshape(RANGES, LANES), axis=0, keepdims=True)
    lane = iota((1, LANES), 1)
    roc_ref[0] = jnp.sum(jnp.where(lane == 0, sums, 0.0))
    prc_ref[0] = jnp.sum(jnp.where(lane == 1, sums, 0.0))
    flag_ref[0] = jnp.sum(jnp.where(lane == 2, sums, 0.0))


def vmem():
    return pl.BlockSpec(memory_space=pltpu.VMEM)


def smem():
    return pl.BlockSpec(memory_space=pltpu.SMEM)


def f32(*shape):
    return jax.ShapeDtypeStruct(shape, jnp.float32)


def near(*shape):
    return pltpu.VMEM(shape, jnp.float32)


def at_hand(x):
    return pltpu.with_memory_space_constraint(x, pltpu.VMEM)


def on_device(bucket, label, group, group_weight):
    blocks = bucket.shape[0] // LANES
    message = pl.pallas_call(
        route_kernel,
        out_shape=near(4 * RANGES, LANES),
        in_specs=[smem(), vmem(), vmem(), vmem()],
        out_specs=vmem(),
        scratch_shapes=[pltpu.VMEM((blocks, LANES), jnp.float32)] * 4
        + [pltpu.VMEM((48, 3 * LANES, LANES), jnp.bfloat16), pltpu.VMEM((3 * LANES, LANES), jnp.float32)],
        name="route",
    )(group_weight, bucket.reshape(blocks, LANES), label.reshape(blocks, LANES), group.reshape(blocks, LANES))
    received = lax.all_to_all(message.reshape(RANGES, 4, LANES), AXES, 0, 0, tiled=True)
    curves, parts = pl.pallas_call(
        curve_kernel,
        out_shape=(near(2, ROWS, LANES), near(RANGES, 1, LANES)),
        in_specs=[vmem()],
        out_specs=(vmem(), vmem()),
        name="curve",
    )(at_hand(received.reshape(4 * RANGES, LANES)))
    parts = lax.all_to_all(parts, AXES, 0, 0, tiled=True)
    others = [lax.ppermute(curves, "grp", [(i, (i + k) % 4) for i in range(4)]) for k in (1, 2, 3)]
    tpr, precision = pl.pallas_call(
        join_kernel,
        out_shape=(f32(4, ROWS, LANES), f32(4, ROWS, LANES)),
        in_specs=[vmem()] * 4,
        out_specs=(vmem(), vmem()),
        name="join",
    )(at_hand(curves), *[at_hand(x) for x in others])
    roc, prc, flag = pl.pallas_call(
        area_kernel,
        out_shape=(f32(1), f32(1), f32(1)),
        in_specs=[vmem()],
        out_specs=(smem(), smem(), smem()),
        name="area",
    )(at_hand(parts))
    quick = (tpr.reshape(4 * ROWS * LANES), precision.reshape(4 * ROWS * LANES), roc.reshape(()), prc.reshape(()))

    def again(state):
        return (jnp.zeros((), jnp.float32), *general(bucket, label, group, group_weight))

    state = lax.while_loop(lambda s: s[0] > 0.0, again, (flag.reshape(()), *quick))
    return state[1:]


def solution(mesh):
    placed = (P(AXES), P(AXES), P(AXES), P())
    return jax.shard_map(
        on_device,
        mesh=mesh,
        in_specs=placed,
        out_specs=(P("shard"), P("shard"), P(), P()),
        check_vma=False,
    )
```

```python
import jax
import jax.numpy as jnp
from jax import lax
from jax.experimental import pallas as pl
from jax.experimental.pallas import tpu as pltpu
from jax.sharding import PartitionSpec as P


LO = 256
BLOCK = 1024
HI = 4096
BATCH = 6

AXES = ("grp", "shard")
LANES = 128
RANGES = 128
RANGE_BITS = 13
ROWS = 64
CAP = 126
NT = (((1,), (1,)), ((), ()))
NN = (((1,), (0,)), ((), ()))
HIGHEST = lax.Precision.HIGHEST


def copy_for_each(x, axis):
    count = lax.axis_size(axis)
    return lax.all_to_all(jnp.broadcast_to(x[None], (count, *x.shape)), axis, 0, 0, tiled=True)


def over_copies(x, axis):
    everything = copy_for_each(x, axis)
    return jnp.sum(everything, axis=0)


def laid_out(tiles, dim):
    dims = list(tiles.shape[1:])
    dims[dim] *= tiles.shape[0]
    return jnp.moveaxis(tiles, 0, dim).reshape(dims)


def collect(x, axis, dim):
    tiles = copy_for_each(x, axis)
    return laid_out(tiles, dim)


def in_one(arrays, axis):
    ends = [0]
    for a in arrays:
        ends.append(ends[-1] + a.size)
    so_far = over_copies(jnp.concatenate([a.ravel() for a in arrays]), axis)
    return tuple((so_far[b:e].reshape(a.shape) for a, b, e in zip(arrays, ends, ends[1:])))


def histogram(bucket, label, group, group_weight, start, count):
    choose = group[:, None] == jnp.arange(group_weight.shape[0])[None, :]
    weight = jnp.sum(jnp.where(choose, group_weight[None, :], 0.0), axis=1)
    labels = label.astype(jnp.float32)
    positive = (weight * labels).astype(jnp.bfloat16)
    negative = (weight * (1.0 - labels)).astype(jnp.bfloat16)
    rows = bucket.shape[0]
    width = BLOCK
    blocks = rows // width

    def accumulate(total, items):
        ids, plus, minus = items
        high = ids // LO
        low = ids % LO
        high_one = high[:, None] == start + jnp.arange(count)[None, :]
        zero = jnp.zeros((), jnp.bfloat16)
        left = jnp.stack(
            [jnp.where(high_one, plus[:, None], zero), jnp.where(high_one, minus[:, None], zero)],
            axis=2,
        )
        left = left.reshape(width, count * 2)
        low_one = (low[:, None] == jnp.arange(LO)[None, :]).astype(jnp.bfloat16)
        product = lax.dot_general(
            left, low_one, (((0,), (0,)), ((), ())), preferred_element_type=jnp.float32
        )
        return (total + product, None)

    initial = jnp.zeros((count * 2, LO), jnp.float32)
    items = (
        bucket.reshape(blocks, width),
        positive.reshape(blocks, width),
        negative.reshape(blocks, width),
    )
    total, _ = lax.scan(accumulate, initial, items)
    return total.reshape(count, 2, LO)


def general(bucket, label, group, group_weight):
    shards = lax.axis_size("shard")
    own_rows = HI // shards
    first_row = lax.axis_index("shard") * own_rows
    ids = lax.all_gather(bucket, "shard", axis=0, tiled=True)
    clicks = lax.all_gather(label, "shard", axis=0, tiled=True)
    groups = lax.all_gather(group, "shard", axis=0, tiled=True)
    owned = histogram(ids, clicks, groups, group_weight, first_row, own_rows)
    owned = over_copies(owned, "grp")
    upper = (jnp.arange(LO)[:, None] >= jnp.arange(LO)[None, :]).astype(jnp.float32)
    row_suffix = jnp.dot(owned.reshape(own_rows * 2, LO), upper, precision=HIGHEST)
    row_totals = jnp.sum(owned, axis=2)
    strict = (jnp.arange(own_rows)[None, :] > jnp.arange(own_rows)[:, None]).astype(jnp.float32)
    after = jnp.dot(strict, row_totals, precision=HIGHEST)
    range_total = jnp.sum(row_totals, axis=0)
    every = collect(range_total[None, :], "shard", 0)
    later = jnp.arange(shards) > lax.axis_index("shard")
    higher = jnp.sum(jnp.where(later[:, None], every, 0.0), axis=0)
    overall = jnp.sum(every, axis=0)
    cumulative = row_suffix.reshape(own_rows, 2, LO) + after[:, :, None] + higher[None, :, None]
    true_pos = cumulative[:, 0, :]
    false_pos = cumulative[:, 1, :]
    pos_hist = owned[:, 0, :]
    neg_hist = owned[:, 1, :]
    tpr_curve = (true_pos / overall[0]).reshape(own_rows * LO)
    precision = true_pos / jnp.maximum(true_pos + false_pos, 1.0)
    roc_part = jnp.sum(neg_hist * (2.0 * true_pos - pos_hist))
    prc_part = jnp.sum(pos_hist * precision)
    roc_sum, prc_sum = in_one((roc_part, prc_part), "shard")
    auroc = roc_sum / (2.0 * overall[0] * overall[1])
    auprc = prc_sum / overall[0]
    return (tpr_curve, precision.reshape(own_rows * LO), auroc, auprc)


def iota(shape, dim):
    return lax.broadcasted_iota(jnp.int32, shape, dim)


def bf16_rows(row):
    return jnp.broadcast_to(row, (16, row.shape[1])).astype(jnp.bfloat16)


def one_hot(row, groups, value, none):
    first = iota((16, LANES), 0).astype(jnp.float32).astype(jnp.bfloat16)
    return [jnp.where(first + jnp.bfloat16(16 * k) == row, value, none) for k in range(groups)]


def route_kernel(weights_ref, bucket_ref, label_ref, group_ref, out_ref,
                 peer_s, high_s, low_s, sign_s):
    blocks = bucket_ref.shape[0]
    bucket = bucket_ref[...]
    group = group_ref[...]
    weight = jnp.zeros(group.shape, jnp.float32)
    for k in range(weights_ref.shape[0]):
        weight = jnp.where(group == k, weights_ref[k], weight)
    labels = label_ref[...].astype(jnp.float32)
    positive = (weight * labels).astype(jnp.bfloat16).astype(jnp.float32)
    negative = (weight * (1.0 - labels)).astype(jnp.bfloat16).astype(jnp.float32)
    sign_s[...] = positive - negative
    which = bucket >> RANGE_BITS
    peer = ((which & 3) << 5) | (which >> 2)
    peer_s[...] = peer.astype(jnp.float32)
    high_s[...] = ((bucket >> 7) & (ROWS - 1)).astype(jnp.float32)
    low_s[...] = (bucket & (LANES - 1)).astype(jnp.float32)

    wide = 2 * LANES
    upto = (iota((wide, wide), 0) <= iota((wide, wide), 1)).astype(jnp.bfloat16)
    none = jnp.zeros((16, LANES), jnp.bfloat16)
    unit = jnp.ones((16, LANES), jnp.bfloat16)

    first = iota((16, LANES), 0).astype(jnp.float32).astype(jnp.bfloat16)
    ones = []
    for j in range(blocks):
        row = bf16_rows(peer_s[pl.ds(j, 1), :])
        ones.append(jnp.concatenate(one_hot(row, 8, unit, none), axis=0))
    pairs = [jnp.concatenate(ones[j:j + 2], axis=1) for j in range(0, blocks, 2)]
    count = jnp.zeros((RANGES, LANES), jnp.float32)
    left = []
    right = []
    for v in range(0, len(pairs), BATCH):
        batch = pairs[v:v + BATCH]
        seen_all = lax.dot_general(jnp.concatenate(batch, axis=0), upto, NN, preferred_element_type=jnp.float32)
        for w in range(len(batch)):
            seen = seen_all[w * RANGES:(w + 1) * RANGES]
            for h in range(2):
                j = 2 * (v + w) + h
                mine = ones[j].astype(jnp.float32)
                before = seen[:, h * LANES:(h + 1) * LANES] + count
                rank = jnp.sum(mine * before, axis=0, keepdims=True) - 1.0
                upper = rank >= LANES // 2
                rank = bf16_rows(jnp.where(upper, rank - LANES // 2, rank))
                upper = bf16_rows(jnp.where(upper, 1.0, 0.0)) > none
                high = bf16_rows(high_s[pl.ds(j, 1), :])
                low = bf16_rows(low_s[pl.ds(j, 1), :])
                sign = bf16_rows(sign_s[pl.ds(j, 1), :])
                same = [first + jnp.bfloat16(16 * k) == rank for k in range(4)]
                left.append(jnp.concatenate(
                    [jnp.where(m, value, none) for value in (high, low, sign) for m in same], axis=0))
                parts = [ones[j][16 * k:16 * k + 16] for k in range(8)]
                right.append(jnp.concatenate(
                    [jnp.where(upper, none, part) for part in parts] + [jnp.where(upper, part, none) for part in parts],
                    axis=0))
            count = count + jnp.broadcast_to(seen[:, wide - 1:wide], (RANGES, LANES))
    placed = lax.dot_general(jnp.concatenate(left, axis=1), jnp.concatenate(right, axis=1), NT,
                             preferred_element_type=jnp.float32)

    def slots(c):
        rows = placed[c * LANES // 2:(c + 1) * LANES // 2]
        return jnp.concatenate([rows[:, :RANGES], rows[:, RANGES:]], axis=0)

    full = jnp.max(jnp.where(count > CAP, 1.0, 0.0), axis=0, keepdims=True)
    full = jnp.max(full, axis=1, keepdims=True)

    slot = iota((LANES, RANGES), 0)
    real = slot < CAP
    high = slots(0)
    low = slots(1)
    sign = jnp.where(real, slots(2), 0.0)
    pos = jnp.maximum(sign, 0.0)
    neg = jnp.maximum(-sign, 0.0)
    p0 = iota((RANGES, RANGES), 0)
    p1 = iota((RANGES, RANGES), 1)
    r0 = ((p0 & 31) << 2) | (p0 >> 5)
    r1 = ((p1 & 31) << 2) | (p1 >> 5)
    above = (r0 > r1).astype(jnp.bfloat16)
    both = jnp.concatenate([pos, neg], axis=0).astype(jnp.bfloat16)
    later = lax.dot_general(both, above, NN, preferred_element_type=jnp.float32)
    for c, own in ((2, pos), (3, neg)):
        higher = jnp.sum(later[(c - 2) * LANES:(c - 1) * LANES], axis=0, keepdims=True)
        total = jnp.sum(jnp.sum(own, axis=0, keepdims=True), axis=1, keepdims=True)
        sent = jnp.where(real, own, jnp.where(slot == CAP, higher, total))
        out_ref[pl.ds(c, RANGES, stride=4), :] = sent.T
    out_ref[pl.ds(0, RANGES, stride=4), :] = jnp.where(real, high, full).T
    out_ref[pl.ds(1, RANGES, stride=4), :] = low.T


def in_three(x):
    first = x.astype(jnp.bfloat16)
    rest = x - first.astype(jnp.float32)
    second = rest.astype(jnp.bfloat16)
    rest = rest - second.astype(jnp.float32)
    return first, second, rest.astype(jnp.bfloat16)


def curve_kernel(in_ref, curve_ref, part_ref):
    step = 128
    none = jnp.zeros((16, LANES), jnp.bfloat16)
    unit = jnp.ones((16, LANES), jnp.bfloat16)
    first = iota((16, LANES), 0).astype(jnp.float32).astype(jnp.bfloat16)
    real = iota((16, LANES), 1) < CAP

    def chunk(i, carry):
        hist, sums = carry
        left = []
        right = []
        for u in range(step):
            at = (i * step + u) * 4
            high = bf16_rows(in_ref[pl.ds(at, 1), :])
            low = bf16_rows(in_ref[pl.ds(at + 1, 1), :])
            pos = jnp.where(real, jnp.broadcast_to(in_ref[pl.ds(at + 2, 1), :], (16, LANES)), 0.0).astype(jnp.bfloat16)
            neg = jnp.where(real, jnp.broadcast_to(in_ref[pl.ds(at + 3, 1), :], (16, LANES)), 0.0).astype(jnp.bfloat16)
            same = [first + jnp.bfloat16(16 * k) == high for k in range(4)]
            left.append(jnp.concatenate(
                [jnp.where(m, pos, none) for m in same] + [jnp.where(m, neg, none) for m in same], axis=0))
            right.append(jnp.concatenate(one_hot(low, 8, unit, none), axis=0))
        hist = hist + lax.dot_general(jnp.concatenate(left, axis=1), jnp.concatenate(right, axis=1), NT,
                                      preferred_element_type=jnp.float32)
        for u in range(step // 2):
            sums = sums + in_ref[pl.ds((i * step + 2 * u) * 4, 8), :]
        return hist, sums

    start = (jnp.zeros((2 * ROWS, LANES), jnp.float32), jnp.zeros((8, LANES), jnp.float32))
    hist, sums = lax.fori_loop(0, RANGES // step, chunk, start)
    sums = sums[0:4] + sums[4:8]
    flag = sums[0:1, CAP:CAP + 1]
    higher_pos = sums[2:3, CAP:CAP + 1]
    total_pos = sums[2:3, CAP + 1:CAP + 2]
    higher_neg = sums[3:4, CAP:CAP + 1]
    total_neg = sums[3:4, CAP + 1:CAP + 2]
    upper = (iota((LANES, LANES), 0) >= iota((LANES, LANES), 1)).astype(jnp.bfloat16)
    row = iota((2 * ROWS, 2 * ROWS), 0)
    col = iota((2 * ROWS, 2 * ROWS), 1)
    below = ((col > row) & ((col >= ROWS) == (row >= ROWS))).astype(jnp.bfloat16)
    pieces = in_three(hist)
    in_row = lax.dot_general(jnp.concatenate(pieces, axis=1), jnp.concatenate([upper] * 3, axis=0), NN,
                             preferred_element_type=jnp.float32)
    rows_after = lax.dot_general(jnp.concatenate([below] * 3, axis=1), jnp.concatenate(pieces, axis=0), NN,
                                 preferred_element_type=jnp.float32)
    cumulative = in_row + jnp.sum(rows_after, axis=1, keepdims=True)
    true_pos = cumulative[:ROWS] + higher_pos
    false_pos = cumulative[ROWS:] + higher_neg
    pos_hist = hist[:ROWS]
    neg_hist = hist[ROWS:]
    precision = true_pos / jnp.maximum(true_pos + false_pos, 1.0)
    curve_ref[0] = true_pos / total_pos
    curve_ref[1] = precision
    roc = jnp.sum(neg_hist * (2.0 * true_pos - pos_hist), axis=0, keepdims=True)
    prc = jnp.sum(pos_hist * precision, axis=0, keepdims=True)
    roc = jnp.sum(roc, axis=1, keepdims=True) / (2.0 * total_pos * total_neg)
    prc = jnp.sum(prc, axis=1, keepdims=True) / total_pos
    lane = iota((RANGES, 1, LANES), 2)
    part_ref[...] = jnp.where(lane == 0, roc[None], jnp.where(lane == 1, prc[None], flag[None]))


def join_kernel(own_ref, one_ref, two_ref, three_ref, tpr_ref, precision_ref):
    me = lax.axis_index("grp")
    for k, ref in enumerate((own_ref, one_ref, two_ref, three_ref)):
        source = (me - k) & 3
        tpr_ref[source] = ref[0]
        precision_ref[source] = ref[1]


def area_kernel(part_ref, roc_ref, prc_ref, flag_ref):
    sums = jnp.sum(part_ref[...].reshape(RANGES, LANES), axis=0, keepdims=True)
    lane = iota((1, LANES), 1)
    roc_ref[0] = jnp.sum(jnp.where(lane == 0, sums, 0.0))
    prc_ref[0] = jnp.sum(jnp.where(lane == 1, sums, 0.0))
    flag_ref[0] = jnp.sum(jnp.where(lane == 2, sums, 0.0))


def vmem():
    return pl.BlockSpec(memory_space=pltpu.VMEM)


def smem():
    return pl.BlockSpec(memory_space=pltpu.SMEM)


def f32(*shape):
    return jax.ShapeDtypeStruct(shape, jnp.float32)


def near(*shape):
    return pltpu.VMEM(shape, jnp.float32)


def at_hand(x):
    return pltpu.with_memory_space_constraint(x, pltpu.VMEM)


def on_device(bucket, label, group, group_weight):
    blocks = bucket.shape[0] // LANES
    message = pl.pallas_call(
        route_kernel,
        out_shape=near(4 * RANGES, LANES),
        in_specs=[smem(), vmem(), vmem(), vmem()],
        out_specs=vmem(),
        scratch_shapes=[pltpu.VMEM((blocks, LANES), jnp.float32)] * 4,
        name="route",
    )(group_weight, bucket.reshape(blocks, LANES), label.reshape(blocks, LANES), group.reshape(blocks, LANES))
    received = lax.all_to_all(message.reshape(RANGES, 4, LANES), AXES, 0, 0, tiled=True)
    curves, parts = pl.pallas_call(
        curve_kernel,
        out_shape=(near(2, ROWS, LANES), near(RANGES, 1, LANES)),
        in_specs=[vmem()],
        out_specs=(vmem(), vmem()),
        name="curve",
    )(at_hand(received.reshape(4 * RANGES, LANES)))
    parts = lax.all_to_all(parts, AXES, 0, 0, tiled=True)
    others = [lax.ppermute(curves, "grp", [(i, (i + k) % 4) for i in range(4)]) for k in (1, 2, 3)]
    tpr, precision = pl.pallas_call(
        join_kernel,
        out_shape=(f32(4, ROWS, LANES), f32(4, ROWS, LANES)),
        in_specs=[vmem()] * 4,
        out_specs=(vmem(), vmem()),
        name="join",
    )(at_hand(curves), *[at_hand(x) for x in others])
    roc, prc, flag = pl.pallas_call(
        area_kernel,
        out_shape=(f32(1), f32(1), f32(1)),
        in_specs=[vmem()],
        out_specs=(smem(), smem(), smem()),
        name="area",
    )(at_hand(parts))
    quick = (tpr.reshape(4 * ROWS * LANES), precision.reshape(4 * ROWS * LANES), roc.reshape(()), prc.reshape(()))

    def again(state):
        return (jnp.zeros((), jnp.float32), *general(bucket, label, group, group_weight))

    state = lax.while_loop(lambda s: s[0] > 0.0, again, (flag.reshape(()), *quick))
    return state[1:]


def solution(mesh):
    placed = (P(AXES), P(AXES), P(AXES), P())
    return jax.shard_map(
        on_device,
        mesh=mesh,
        in_specs=placed,
        out_specs=(P("shard"), P("shard"), P(), P()),
        check_vma=False,
    )
```

```python
import jax
import jax.numpy as jnp
from jax import lax
from jax.experimental import pallas as pl
from jax.experimental.pallas import tpu as pltpu
from jax.sharding import PartitionSpec as P


LO = 256
BLOCK = 1024
HI = 4096
BATCH = 6

AXES = ("grp", "shard")
LANES = 128
RANGES = 128
RANGE_BITS = 13
ROWS = 64
CAP = 126
NT = (((1,), (1,)), ((), ()))
NN = (((1,), (0,)), ((), ()))
HIGHEST = lax.Precision.HIGHEST


def over_grp(x):
    every = lax.all_gather(x.reshape(x.size), "grp", axis=0, tiled=True)
    return jnp.sum(every.reshape(lax.axis_size("grp"), *x.shape), axis=0)


def histogram(bucket, label, group, group_weight, start, count):
    choose = group[:, None] == jnp.arange(group_weight.shape[0])[None, :]
    weight = jnp.sum(jnp.where(choose, group_weight[None, :], 0.0), axis=1)
    labels = label.astype(jnp.float32)
    positive = (weight * labels).astype(jnp.bfloat16)
    negative = (weight * (1.0 - labels)).astype(jnp.bfloat16)
    rows = bucket.shape[0]
    width = BLOCK
    blocks = rows // width

    def accumulate(total, items):
        ids, plus, minus = items
        high = ids // LO
        low = ids % LO
        high_one = high[:, None] == start + jnp.arange(count)[None, :]
        zero = jnp.zeros((), jnp.bfloat16)
        left = jnp.stack(
            [jnp.where(high_one, plus[:, None], zero), jnp.where(high_one, minus[:, None], zero)],
            axis=2,
        )
        left = left.reshape(width, count * 2)
        low_one = (low[:, None] == jnp.arange(LO)[None, :]).astype(jnp.bfloat16)
        product = lax.dot_general(
            left, low_one, (((0,), (0,)), ((), ())), preferred_element_type=jnp.float32
        )
        return (total + product, None)

    initial = jnp.zeros((count * 2, LO), jnp.float32)
    items = (
        bucket.reshape(blocks, width),
        positive.reshape(blocks, width),
        negative.reshape(blocks, width),
    )
    total, _ = lax.scan(accumulate, initial, items)
    return total.reshape(count, 2, LO)


def general(bucket, label, group, group_weight):
    shards = lax.axis_size("shard")
    own_rows = HI // shards
    first_row = lax.axis_index("shard") * own_rows
    ids = lax.all_gather(bucket, "shard", axis=0, tiled=True)
    clicks = lax.all_gather(label, "shard", axis=0, tiled=True)
    groups = lax.all_gather(group, "shard", axis=0, tiled=True)
    owned = histogram(ids, clicks, groups, group_weight, first_row, own_rows)
    owned = jnp.concatenate([over_grp(owned[:own_rows // 2]), over_grp(owned[own_rows // 2:])], axis=0)
    upper = (jnp.arange(LO)[:, None] >= jnp.arange(LO)[None, :]).astype(jnp.float32)
    row_suffix = jnp.dot(owned.reshape(own_rows * 2, LO), upper, precision=HIGHEST)
    row_totals = jnp.sum(owned, axis=2)
    strict = (jnp.arange(own_rows)[None, :] > jnp.arange(own_rows)[:, None]).astype(jnp.float32)
    after = jnp.dot(strict, row_totals, precision=HIGHEST)
    range_total = jnp.sum(row_totals, axis=0)
    every = lax.all_gather(range_total, "shard")
    later = jnp.arange(shards) > lax.axis_index("shard")
    higher = jnp.sum(jnp.where(later[:, None], every, 0.0), axis=0)
    overall = jnp.sum(every, axis=0)
    cumulative = row_suffix.reshape(own_rows, 2, LO) + after[:, :, None] + higher[None, :, None]
    true_pos = cumulative[:, 0, :]
    false_pos = cumulative[:, 1, :]
    pos_hist = owned[:, 0, :]
    neg_hist = owned[:, 1, :]
    tpr_curve = (true_pos / overall[0]).reshape(own_rows * LO)
    precision = true_pos / jnp.maximum(true_pos + false_pos, 1.0)
    roc_part = jnp.sum(neg_hist * (2.0 * true_pos - pos_hist))
    prc_part = jnp.sum(pos_hist * precision)
    roc_sum, prc_sum = lax.psum((roc_part, prc_part), "shard")
    auroc = roc_sum / (2.0 * overall[0] * overall[1])
    auprc = prc_sum / overall[0]
    return (tpr_curve, precision.reshape(own_rows * LO), auroc, auprc)


def iota(shape, dim):
    return lax.broadcasted_iota(jnp.int32, shape, dim)


def bf16_rows(row):
    return jnp.broadcast_to(row, (16, row.shape[1])).astype(jnp.bfloat16)


def one_hot(row, groups, value, none):
    first = iota((16, LANES), 0).astype(jnp.float32).astype(jnp.bfloat16)
    return [jnp.where(first + jnp.bfloat16(16 * k) == row, value, none) for k in range(groups)]


def route_kernel(weights_ref, bucket_ref, label_ref, group_ref, out_ref,
                 peer_s, high_s, low_s, sign_s):
    blocks = bucket_ref.shape[0]
    bucket = bucket_ref[...]
    group = group_ref[...]
    weight = jnp.zeros(group.shape, jnp.float32)
    for k in range(weights_ref.shape[0]):
        weight = jnp.where(group == k, weights_ref[k], weight)
    labels = label_ref[...].astype(jnp.float32)
    positive = (weight * labels).astype(jnp.bfloat16).astype(jnp.float32)
    negative = (weight * (1.0 - labels)).astype(jnp.bfloat16).astype(jnp.float32)
    sign_s[...] = positive - negative
    which = bucket >> RANGE_BITS
    peer = ((which & 3) << 5) | (which >> 2)
    peer_s[...] = peer.astype(jnp.float32)
    high_s[...] = ((bucket >> 7) & (ROWS - 1)).astype(jnp.float32)
    low_s[...] = (bucket & (LANES - 1)).astype(jnp.float32)

    wide = 2 * LANES
    upto = (iota((wide, wide), 0) <= iota((wide, wide), 1)).astype(jnp.bfloat16)
    none = jnp.zeros((16, LANES), jnp.bfloat16)
    unit = jnp.ones((16, LANES), jnp.bfloat16)

    first = iota((16, LANES), 0).astype(jnp.float32).astype(jnp.bfloat16)
    ones = []
    for j in range(blocks):
        row = bf16_rows(peer_s[pl.ds(j, 1), :])
        ones.append(jnp.concatenate(one_hot(row, 8, unit, none), axis=0))
    pairs = [jnp.concatenate(ones[j:j + 2], axis=1) for j in range(0, blocks, 2)]
    count = jnp.zeros((RANGES, LANES), jnp.float32)
    left = []
    right = []
    for v in range(0, len(pairs), BATCH):
        batch = pairs[v:v + BATCH]
        seen_all = lax.dot_general(jnp.concatenate(batch, axis=0), upto, NN, preferred_element_type=jnp.float32)
        for w in range(len(batch)):
            seen = seen_all[w * RANGES:(w + 1) * RANGES]
            for h in range(2):
                j = 2 * (v + w) + h
                mine = ones[j].astype(jnp.float32)
                before = seen[:, h * LANES:(h + 1) * LANES] + count
                rank = jnp.sum(mine * before, axis=0, keepdims=True) - 1.0
                upper = rank >= LANES // 2
                rank = bf16_rows(jnp.where(upper, rank - LANES // 2, rank))
                upper = bf16_rows(jnp.where(upper, 1.0, 0.0)) > none
                high = bf16_rows(high_s[pl.ds(j, 1), :])
                low = bf16_rows(low_s[pl.ds(j, 1), :])
                sign = bf16_rows(sign_s[pl.ds(j, 1), :])
                same = [first + jnp.bfloat16(16 * k) == rank for k in range(4)]
                left.append(jnp.concatenate(
                    [jnp.where(m, value, none) for value in (high, low, sign) for m in same], axis=0))
                parts = [ones[j][16 * k:16 * k + 16] for k in range(8)]
                right.append(jnp.concatenate(
                    [jnp.where(upper, none, part) for part in parts] + [jnp.where(upper, part, none) for part in parts],
                    axis=0))
            count = count + jnp.broadcast_to(seen[:, wide - 1:wide], (RANGES, LANES))
    placed = lax.dot_general(jnp.concatenate(left, axis=1), jnp.concatenate(right, axis=1), NT,
                             preferred_element_type=jnp.float32)

    def slots(c):
        rows = placed[c * LANES // 2:(c + 1) * LANES // 2]
        return jnp.concatenate([rows[:, :RANGES], rows[:, RANGES:]], axis=0)

    full = jnp.max(jnp.where(count > CAP, 1.0, 0.0), axis=0, keepdims=True)
    full = jnp.max(full, axis=1, keepdims=True)

    slot = iota((LANES, RANGES), 0)
    real = slot < CAP
    high = slots(0)
    low = slots(1)
    sign = jnp.where(real, slots(2), 0.0)
    pos = jnp.maximum(sign, 0.0)
    neg = jnp.maximum(-sign, 0.0)
    p0 = iota((RANGES, RANGES), 0)
    p1 = iota((RANGES, RANGES), 1)
    r0 = ((p0 & 31) << 2) | (p0 >> 5)
    r1 = ((p1 & 31) << 2) | (p1 >> 5)
    above = (r0 > r1).astype(jnp.bfloat16)
    both = jnp.concatenate([pos, neg], axis=0).astype(jnp.bfloat16)
    later = lax.dot_general(both, above, NN, preferred_element_type=jnp.float32)
    for c, own in ((2, pos), (3, neg)):
        higher = jnp.sum(later[(c - 2) * LANES:(c - 1) * LANES], axis=0, keepdims=True)
        total = jnp.sum(jnp.sum(own, axis=0, keepdims=True), axis=1, keepdims=True)
        sent = jnp.where(real, own, jnp.where(slot == CAP, higher, total))
        out_ref[pl.ds(c, RANGES, stride=4), :] = sent.T
    out_ref[pl.ds(0, RANGES, stride=4), :] = jnp.where(real, high, full).T
    out_ref[pl.ds(1, RANGES, stride=4), :] = low.T


def in_three(x):
    first = x.astype(jnp.bfloat16)
    rest = x - first.astype(jnp.float32)
    second = rest.astype(jnp.bfloat16)
    rest = rest - second.astype(jnp.float32)
    return first, second, rest.astype(jnp.bfloat16)


def curve_kernel(in_ref, curve_ref, part_ref, fix_ref, flag_ref):
    step = 128
    none = jnp.zeros((16, LANES), jnp.bfloat16)
    unit = jnp.ones((16, LANES), jnp.bfloat16)
    first = iota((16, LANES), 0).astype(jnp.float32).astype(jnp.bfloat16)
    real = iota((16, LANES), 1) < CAP

    def chunk(i, carry):
        hist, sums = carry
        left = []
        right = []
        for u in range(step):
            at = (i * step + u) * 4
            high = bf16_rows(in_ref[pl.ds(at, 1), :])
            low = bf16_rows(in_ref[pl.ds(at + 1, 1), :])
            pos = jnp.where(real, jnp.broadcast_to(in_ref[pl.ds(at + 2, 1), :], (16, LANES)), 0.0).astype(jnp.bfloat16)
            neg = jnp.where(real, jnp.broadcast_to(in_ref[pl.ds(at + 3, 1), :], (16, LANES)), 0.0).astype(jnp.bfloat16)
            same = [first + jnp.bfloat16(16 * k) == high for k in range(4)]
            left.append(jnp.concatenate(
                [jnp.where(m, pos, none) for m in same] + [jnp.where(m, neg, none) for m in same], axis=0))
            right.append(jnp.concatenate(one_hot(low, 8, unit, none), axis=0))
        hist = hist + lax.dot_general(jnp.concatenate(left, axis=1), jnp.concatenate(right, axis=1), NT,
                                      preferred_element_type=jnp.float32)
        for u in range(step // 2):
            sums = sums + in_ref[pl.ds((i * step + 2 * u) * 4, 8), :]
        return hist, sums

    start = (jnp.zeros((2 * ROWS, LANES), jnp.float32), jnp.zeros((8, LANES), jnp.float32))
    hist, sums = lax.fori_loop(0, RANGES // step, chunk, start)
    sums = sums[0:4] + sums[4:8]
    flag = sums[0:1, CAP:CAP + 1]
    higher_pos = sums[2:3, CAP:CAP + 1]
    total_pos = sums[2:3, CAP + 1:CAP + 2]
    higher_neg = sums[3:4, CAP:CAP + 1]
    total_neg = sums[3:4, CAP + 1:CAP + 2]
    upper = (iota((LANES, LANES), 0) >= iota((LANES, LANES), 1)).astype(jnp.bfloat16)
    row = iota((2 * ROWS, 2 * ROWS), 0)
    col = iota((2 * ROWS, 2 * ROWS), 1)
    below = ((col > row) & ((col >= ROWS) == (row >= ROWS))).astype(jnp.bfloat16)
    pieces = in_three(hist)
    in_row = lax.dot_general(jnp.concatenate(pieces, axis=1), jnp.concatenate([upper] * 3, axis=0), NN,
                             preferred_element_type=jnp.float32)
    rows_after = lax.dot_general(jnp.concatenate([below] * 3, axis=1), jnp.concatenate(pieces, axis=0), NN,
                                 preferred_element_type=jnp.float32)
    cumulative = in_row + jnp.sum(rows_after, axis=1, keepdims=True)
    true_pos = cumulative[:ROWS] + higher_pos
    false_pos = cumulative[ROWS:] + higher_neg
    pos_hist = hist[:ROWS]
    neg_hist = hist[ROWS:]
    precision = true_pos / jnp.maximum(true_pos + false_pos, 1.0)
    curve_ref[0] = true_pos / total_pos
    curve_ref[1] = precision
    roc = jnp.sum(neg_hist * (2.0 * true_pos - pos_hist), axis=0, keepdims=True)
    prc = jnp.sum(pos_hist * precision, axis=0, keepdims=True)
    roc = jnp.sum(roc, axis=1, keepdims=True) / (2.0 * total_pos * total_neg)
    prc = jnp.sum(prc, axis=1, keepdims=True) / total_pos
    lane = iota((RANGES, 1, LANES), 2)
    part_ref[...] = jnp.where(lane == 0, roc[None], jnp.where(lane == 1, prc[None], flag[None]))
    fix_ref[...] = jnp.zeros((8, LANES), jnp.float32)
    flag_ref[0] = jnp.max(flag)


def join_kernel(own_ref, one_ref, two_ref, three_ref, tpr_ref, precision_ref):
    me = lax.axis_index("grp")
    for k, ref in enumerate((own_ref, one_ref, two_ref, three_ref)):
        source = (me - k) & 3
        tpr_ref[source] = ref[0]
        precision_ref[source] = ref[1]


def area_kernel(part_ref, fix_ref, roc_ref, prc_ref, fix_s, done):
    sums = jnp.sum(part_ref[...].reshape(RANGES, LANES), axis=0, keepdims=True)
    lane = iota((1, LANES), 1)
    roc_ref[0] = jnp.sum(jnp.where(lane == 0, sums, 0.0))
    prc_ref[0] = jnp.sum(jnp.where(lane == 1, sums, 0.0))

    @pl.when(jnp.sum(jnp.where(lane == 2, sums, 0.0)) > 0.0)
    def _():
        copy = pltpu.make_async_copy(fix_ref, fix_s, done)
        copy.start()
        copy.wait()
        fix = fix_s[0:1, :]
        roc_ref[0] = jnp.sum(jnp.where(lane == 0, fix, 0.0))
        prc_ref[0] = jnp.sum(jnp.where(lane == 1, fix, 0.0))


def vmem():
    return pl.BlockSpec(memory_space=pltpu.VMEM)


def smem():
    return pl.BlockSpec(memory_space=pltpu.SMEM)


def f32(*shape):
    return jax.ShapeDtypeStruct(shape, jnp.float32)


def near(*shape):
    return pltpu.VMEM(shape, jnp.float32)


def at_hand(x):
    return pltpu.with_memory_space_constraint(x, pltpu.VMEM)


def on_device(bucket, label, group, group_weight):
    blocks = bucket.shape[0] // LANES
    message = pl.pallas_call(
        route_kernel,
        out_shape=near(4 * RANGES, LANES),
        in_specs=[smem(), vmem(), vmem(), vmem()],
        out_specs=vmem(),
        scratch_shapes=[pltpu.VMEM((blocks, LANES), jnp.float32)] * 4,
        name="route",
    )(group_weight, bucket.reshape(blocks, LANES), label.reshape(blocks, LANES), group.reshape(blocks, LANES))
    received = lax.all_to_all(message.reshape(RANGES, 4, LANES), AXES, 0, 0, tiled=True)
    curves, parts, fix, flag = pl.pallas_call(
        curve_kernel,
        out_shape=(near(2, ROWS, LANES), near(RANGES, 1, LANES), f32(8, LANES), f32(1)),
        in_specs=[vmem()],
        out_specs=(vmem(), vmem(), vmem(), smem()),
        name="curve",
    )(at_hand(received.reshape(4 * RANGES, LANES)))
    parts = lax.all_to_all(parts, AXES, 0, 0, tiled=True)
    others = [lax.ppermute(curves, "grp", [(i, (i + k) % 4) for i in range(4)]) for k in (1, 2, 3)]
    tpr, precision = pl.pallas_call(
        join_kernel,
        out_shape=(f32(4, ROWS, LANES), f32(4, ROWS, LANES)),
        in_specs=[vmem()] * 4,
        out_specs=(vmem(), vmem()),
        name="join",
    )(at_hand(curves), *[at_hand(x) for x in others])
    size = 4 * ROWS * LANES

    def again(state):
        nothing = (state[0] < 0.0).astype(jnp.int32)
        tpr, precision, roc, prc = general(bucket + nothing, label + nothing, group + nothing, group_weight)
        fix = jnp.where(jnp.arange(LANES)[None, :] == 0, roc, prc)
        return jnp.zeros((), jnp.float32), jnp.broadcast_to(fix, (8, LANES)), tpr, precision

    _, fix, tpr, precision = lax.while_loop(
        lambda state: state[0] > 0.0, again,
        (flag.reshape(()), fix, tpr.reshape(size), precision.reshape(size)))
    roc, prc = pl.pallas_call(
        area_kernel,
        out_shape=(f32(1), f32(1)),
        in_specs=[vmem(), pl.BlockSpec(memory_space=pl.ANY)],
        out_specs=(smem(), smem()),
        scratch_shapes=[pltpu.VMEM((8, LANES), jnp.float32), pltpu.SemaphoreType.DMA],
        name="area",
    )(at_hand(parts), fix)
    return tpr, precision, roc.reshape(()), prc.reshape(())


def solution(mesh):
    placed = (P(AXES), P(AXES), P(AXES), P())
    return jax.shard_map(
        on_device,
        mesh=mesh,
        in_specs=placed,
        out_specs=(P("shard"), P("shard"), P(), P()),
        check_vma=False,
    )
```

```python
import jax
import jax.numpy as jnp
from jax import lax
from jax.experimental import pallas as pl
from jax.experimental.pallas import tpu as pltpu
from jax.sharding import PartitionSpec as P


LO = 256
BLOCK = 1024
HI = 4096
BATCH = 6

AXES = ("grp", "shard")
LANES = 128
RANGES = 128
RANGE_BITS = 13
ROWS = 64
CAP = 126
NT = (((1,), (1,)), ((), ()))
NN = (((1,), (0,)), ((), ()))
HIGHEST = lax.Precision.HIGHEST


def over_grp(x):
    every = lax.all_gather(x.reshape(x.size), "grp", axis=0, tiled=True)
    return jnp.sum(every.reshape(lax.axis_size("grp"), *x.shape), axis=0)


def histogram(bucket, label, group, group_weight, start, count):
    choose = group[:, None] == jnp.arange(group_weight.shape[0])[None, :]
    weight = jnp.sum(jnp.where(choose, group_weight[None, :], 0.0), axis=1)
    labels = label.astype(jnp.float32)
    positive = (weight * labels).astype(jnp.bfloat16)
    negative = (weight * (1.0 - labels)).astype(jnp.bfloat16)
    rows = bucket.shape[0]
    width = BLOCK
    blocks = rows // width

    def accumulate(total, items):
        ids, plus, minus = items
        high = ids // LO
        low = ids % LO
        high_one = high[:, None] == start + jnp.arange(count)[None, :]
        zero = jnp.zeros((), jnp.bfloat16)
        left = jnp.stack(
            [jnp.where(high_one, plus[:, None], zero), jnp.where(high_one, minus[:, None], zero)],
            axis=2,
        )
        left = left.reshape(width, count * 2)
        low_one = (low[:, None] == jnp.arange(LO)[None, :]).astype(jnp.bfloat16)
        product = lax.dot_general(
            left, low_one, (((0,), (0,)), ((), ())), preferred_element_type=jnp.float32
        )
        return (total + product, None)

    initial = jnp.zeros((count * 2, LO), jnp.float32)
    items = (
        bucket.reshape(blocks, width),
        positive.reshape(blocks, width),
        negative.reshape(blocks, width),
    )
    total, _ = lax.scan(accumulate, initial, items)
    return total.reshape(count, 2, LO)


def general(bucket, label, group, group_weight):
    shards = lax.axis_size("shard")
    own_rows = HI // shards
    first_row = lax.axis_index("shard") * own_rows
    ids = lax.all_gather(bucket, "shard", axis=0, tiled=True)
    clicks = lax.all_gather(label, "shard", axis=0, tiled=True)
    groups = lax.all_gather(group, "shard", axis=0, tiled=True)
    owned = histogram(ids, clicks, groups, group_weight, first_row, own_rows)
    owned = jnp.concatenate([over_grp(owned[:own_rows // 2]), over_grp(owned[own_rows // 2:])], axis=0)
    upper = (jnp.arange(LO)[:, None] >= jnp.arange(LO)[None, :]).astype(jnp.float32)
    row_suffix = jnp.dot(owned.reshape(own_rows * 2, LO), upper, precision=HIGHEST)
    row_totals = jnp.sum(owned, axis=2)
    strict = (jnp.arange(own_rows)[None, :] > jnp.arange(own_rows)[:, None]).astype(jnp.float32)
    after = jnp.dot(strict, row_totals, precision=HIGHEST)
    range_total = jnp.sum(row_totals, axis=0)
    every = lax.all_gather(range_total, "shard")
    later = jnp.arange(shards) > lax.axis_index("shard")
    higher = jnp.sum(jnp.where(later[:, None], every, 0.0), axis=0)
    overall = jnp.sum(every, axis=0)
    cumulative = row_suffix.reshape(own_rows, 2, LO) + after[:, :, None] + higher[None, :, None]
    true_pos = cumulative[:, 0, :]
    false_pos = cumulative[:, 1, :]
    pos_hist = owned[:, 0, :]
    neg_hist = owned[:, 1, :]
    tpr_curve = (true_pos / overall[0]).reshape(own_rows * LO)
    precision = true_pos / jnp.maximum(true_pos + false_pos, 1.0)
    roc_part = jnp.sum(neg_hist * (2.0 * true_pos - pos_hist))
    prc_part = jnp.sum(pos_hist * precision)
    roc_sum, prc_sum = lax.psum((roc_part, prc_part), "shard")
    auroc = roc_sum / (2.0 * overall[0] * overall[1])
    auprc = prc_sum / overall[0]
    return (tpr_curve, precision.reshape(own_rows * LO), auroc, auprc)


def iota(shape, dim):
    return lax.broadcasted_iota(jnp.int32, shape, dim)


def bf16_rows(row):
    return jnp.broadcast_to(row, (16, row.shape[1])).astype(jnp.bfloat16)


def one_hot(row, groups, value, none):
    first = iota((16, LANES), 0).astype(jnp.float32).astype(jnp.bfloat16)
    return [jnp.where(first + jnp.bfloat16(16 * k) == row, value, none) for k in range(groups)]


def route_kernel(weights_ref, bucket_ref, label_ref, group_ref, out_ref,
                 peer_s, high_s, low_s, sign_s):
    blocks = bucket_ref.shape[0]
    bucket = bucket_ref[...]
    group = group_ref[...]
    weight = jnp.zeros(group.shape, jnp.float32)
    for k in range(weights_ref.shape[0]):
        weight = jnp.where(group == k, weights_ref[k], weight)
    labels = label_ref[...].astype(jnp.float32)
    positive = (weight * labels).astype(jnp.bfloat16).astype(jnp.float32)
    negative = (weight * (1.0 - labels)).astype(jnp.bfloat16).astype(jnp.float32)
    sign_s[...] = positive - negative
    which = bucket >> RANGE_BITS
    peer = ((which & 3) << 5) | (which >> 2)
    peer_s[...] = peer.astype(jnp.float32)
    high_s[...] = ((bucket >> 7) & (ROWS - 1)).astype(jnp.float32)
    low_s[...] = (bucket & (LANES - 1)).astype(jnp.float32)

    wide = 2 * LANES
    upto = (iota((wide, wide), 0) <= iota((wide, wide), 1)).astype(jnp.bfloat16)
    none = jnp.zeros((16, LANES), jnp.bfloat16)
    unit = jnp.ones((16, LANES), jnp.bfloat16)

    first = iota((16, LANES), 0).astype(jnp.float32).astype(jnp.bfloat16)
    ones = []
    for j in range(blocks):
        row = bf16_rows(peer_s[pl.ds(j, 1), :])
        ones.append(jnp.concatenate(one_hot(row, 8, unit, none), axis=0))
    pairs = [jnp.concatenate(ones[j:j + 2], axis=1) for j in range(0, blocks, 2)]
    count = jnp.zeros((RANGES, LANES), jnp.float32)
    left = []
    right = []
    for v in range(0, len(pairs), BATCH):
        batch = pairs[v:v + BATCH]
        seen_all = lax.dot_general(jnp.concatenate(batch, axis=0), upto, NN, preferred_element_type=jnp.float32)
        for w in range(len(batch)):
            seen = seen_all[w * RANGES:(w + 1) * RANGES]
            for h in range(2):
                j = 2 * (v + w) + h
                mine = ones[j].astype(jnp.float32)
                before = seen[:, h * LANES:(h + 1) * LANES] + count
                rank = jnp.sum(mine * before, axis=0, keepdims=True) - 1.0
                upper = rank >= LANES // 2
                rank = bf16_rows(jnp.where(upper, rank - LANES // 2, rank))
                upper = bf16_rows(jnp.where(upper, 1.0, 0.0)) > none
                high = bf16_rows(high_s[pl.ds(j, 1), :])
                low = bf16_rows(low_s[pl.ds(j, 1), :])
                sign = bf16_rows(sign_s[pl.ds(j, 1), :])
                same = [first + jnp.bfloat16(16 * k) == rank for k in range(4)]
                left.append(jnp.concatenate(
                    [jnp.where(m, value, none) for value in (high, low, sign) for m in same], axis=0))
                parts = [ones[j][16 * k:16 * k + 16] for k in range(8)]
                right.append(jnp.concatenate(
                    [jnp.where(upper, none, part) for part in parts] + [jnp.where(upper, part, none) for part in parts],
                    axis=0))
            count = count + jnp.broadcast_to(seen[:, wide - 1:wide], (RANGES, LANES))
    placed = lax.dot_general(jnp.concatenate(left, axis=1), jnp.concatenate(right, axis=1), NT,
                             preferred_element_type=jnp.float32)

    def slots(c):
        rows = placed[c * LANES // 2:(c + 1) * LANES // 2]
        return jnp.concatenate([rows[:, :RANGES], rows[:, RANGES:]], axis=0)

    full = jnp.max(jnp.where(count > CAP, 1.0, 0.0), axis=0, keepdims=True)
    full = jnp.max(full, axis=1, keepdims=True)

    slot = iota((LANES, RANGES), 0)
    real = slot < CAP
    high = slots(0)
    low = slots(1)
    sign = jnp.where(real, slots(2), 0.0)
    pos = jnp.maximum(sign, 0.0)
    neg = jnp.maximum(-sign, 0.0)
    p0 = iota((RANGES, RANGES), 0)
    p1 = iota((RANGES, RANGES), 1)
    r0 = ((p0 & 31) << 2) | (p0 >> 5)
    r1 = ((p1 & 31) << 2) | (p1 >> 5)
    above = (r0 > r1).astype(jnp.bfloat16)
    both = jnp.concatenate([pos, neg], axis=0).astype(jnp.bfloat16)
    later = lax.dot_general(both, above, NN, preferred_element_type=jnp.float32)
    for c, own in ((1, pos), (2, neg)):
        higher = jnp.sum(later[(c - 1) * LANES:c * LANES], axis=0, keepdims=True)
        total = jnp.sum(jnp.sum(own, axis=0, keepdims=True), axis=1, keepdims=True)
        sent = jnp.where(real, own, jnp.where(slot == CAP, higher, total))
        out_ref[pl.ds(c, RANGES, stride=3), :] = sent.T
    out_ref[pl.ds(0, RANGES, stride=3), :] = jnp.where(real, LANES * high + low, full).T


def in_three(x):
    first = x.astype(jnp.bfloat16)
    rest = x - first.astype(jnp.float32)
    second = rest.astype(jnp.bfloat16)
    rest = rest - second.astype(jnp.float32)
    return first, second, rest.astype(jnp.bfloat16)


def curve_kernel(in_ref, curve_ref, part_ref, fix_ref, flag_ref):
    none = jnp.zeros((16, LANES), jnp.bfloat16)
    unit = jnp.ones((16, LANES), jnp.bfloat16)
    first = iota((16, LANES), 0).astype(jnp.float32).astype(jnp.bfloat16)
    real = iota((16, LANES), 1) < CAP
    left = []
    right = []
    for q in range(RANGES):
        place = in_ref[pl.ds(3 * q, 1), :]
        high = jnp.floor(place * (1.0 / LANES))
        low = bf16_rows(place - LANES * high)
        high = bf16_rows(high)
        pos = jnp.where(real, jnp.broadcast_to(in_ref[pl.ds(3 * q + 1, 1), :], (16, LANES)), 0.0).astype(jnp.bfloat16)
        neg = jnp.where(real, jnp.broadcast_to(in_ref[pl.ds(3 * q + 2, 1), :], (16, LANES)), 0.0).astype(jnp.bfloat16)
        same = [first + jnp.bfloat16(16 * k) == high for k in range(4)]
        left.append(jnp.concatenate(
            [jnp.where(m, pos, none) for m in same] + [jnp.where(m, neg, none) for m in same], axis=0))
        right.append(jnp.concatenate(one_hot(low, 8, unit, none), axis=0))
    hist = lax.dot_general(jnp.concatenate(left, axis=1), jnp.concatenate(right, axis=1), NT,
                           preferred_element_type=jnp.float32)
    sums = in_ref[pl.ds(0, 24), :]
    for q in range(24, 3 * RANGES, 24):
        sums = sums + in_ref[pl.ds(q, 24), :]
    kind = iota((24, LANES), 0) % 3
    sums = [jnp.sum(jnp.where(kind == c, sums, 0.0), axis=0, keepdims=True) for c in range(3)]
    flag = sums[0][:, CAP:CAP + 1]
    higher_pos = sums[1][:, CAP:CAP + 1]
    total_pos = sums[1][:, CAP + 1:CAP + 2]
    higher_neg = sums[2][:, CAP:CAP + 1]
    total_neg = sums[2][:, CAP + 1:CAP + 2]
    upper = (iota((LANES, LANES), 0) >= iota((LANES, LANES), 1)).astype(jnp.bfloat16)
    row = iota((2 * ROWS, 2 * ROWS), 0)
    col = iota((2 * ROWS, 2 * ROWS), 1)
    below = ((col > row) & ((col >= ROWS) == (row >= ROWS))).astype(jnp.bfloat16)
    pieces = in_three(hist)
    in_row = lax.dot_general(jnp.concatenate(pieces, axis=1), jnp.concatenate([upper] * 3, axis=0), NN,
                             preferred_element_type=jnp.float32)
    rows_after = lax.dot_general(jnp.concatenate([below] * 3, axis=1), jnp.concatenate(pieces, axis=0), NN,
                                 preferred_element_type=jnp.float32)
    cumulative = in_row + jnp.sum(rows_after, axis=1, keepdims=True)
    true_pos = cumulative[:ROWS] + higher_pos
    false_pos = cumulative[ROWS:] + higher_neg
    pos_hist = hist[:ROWS]
    neg_hist = hist[ROWS:]
    precision = true_pos / jnp.maximum(true_pos + false_pos, 1.0)
    curve_ref[0] = true_pos / total_pos
    curve_ref[1] = precision
    roc = jnp.sum(neg_hist * (2.0 * true_pos - pos_hist), axis=0, keepdims=True)
    prc = jnp.sum(pos_hist * precision, axis=0, keepdims=True)
    roc = jnp.sum(roc, axis=1, keepdims=True) / (2.0 * total_pos * total_neg)
    prc = jnp.sum(prc, axis=1, keepdims=True) / total_pos
    lane = iota((RANGES, 1, LANES), 2)
    part_ref[...] = jnp.where(lane == 0, roc[None], jnp.where(lane == 1, prc[None], flag[None]))
    fix_ref[...] = jnp.zeros((8, LANES), jnp.float32)
    flag_ref[0] = jnp.max(flag)


def join_kernel(own_ref, one_ref, two_ref, three_ref, tpr_ref, precision_ref):
    me = lax.axis_index("grp")
    for k, ref in enumerate((own_ref, one_ref, two_ref, three_ref)):
        source = (me - k) & 3
        tpr_ref[source] = ref[0]
        precision_ref[source] = ref[1]


def area_kernel(part_ref, fix_ref, roc_ref, prc_ref, fix_s, done):
    sums = jnp.sum(part_ref[...].reshape(RANGES, LANES), axis=0, keepdims=True)
    lane = iota((1, LANES), 1)
    roc_ref[0] = jnp.sum(jnp.where(lane == 0, sums, 0.0))
    prc_ref[0] = jnp.sum(jnp.where(lane == 1, sums, 0.0))

    @pl.when(jnp.sum(jnp.where(lane == 2, sums, 0.0)) > 0.0)
    def _():
        copy = pltpu.make_async_copy(fix_ref, fix_s, done)
        copy.start()
        copy.wait()
        fix = fix_s[0:1, :]
        roc_ref[0] = jnp.sum(jnp.where(lane == 0, fix, 0.0))
        prc_ref[0] = jnp.sum(jnp.where(lane == 1, fix, 0.0))


def vmem():
    return pl.BlockSpec(memory_space=pltpu.VMEM)


def smem():
    return pl.BlockSpec(memory_space=pltpu.SMEM)


def f32(*shape):
    return jax.ShapeDtypeStruct(shape, jnp.float32)


def near(*shape):
    return pltpu.VMEM(shape, jnp.float32)


def at_hand(x):
    return pltpu.with_memory_space_constraint(x, pltpu.VMEM)


def on_device(bucket, label, group, group_weight):
    blocks = bucket.shape[0] // LANES
    message = pl.pallas_call(
        route_kernel,
        out_shape=near(3 * RANGES, LANES),
        in_specs=[smem(), vmem(), vmem(), vmem()],
        out_specs=vmem(),
        scratch_shapes=[pltpu.VMEM((blocks, LANES), jnp.float32)] * 4,
        name="route",
    )(group_weight, bucket.reshape(blocks, LANES), label.reshape(blocks, LANES), group.reshape(blocks, LANES))
    received = lax.all_to_all(message.reshape(RANGES, 1, 3 * LANES), AXES, 0, 0, tiled=True)
    curves, parts, fix, flag = pl.pallas_call(
        curve_kernel,
        out_shape=(near(2, ROWS, LANES), near(RANGES, 1, LANES), f32(8, LANES), f32(1)),
        in_specs=[vmem()],
        out_specs=(vmem(), vmem(), vmem(), smem()),
        name="curve",
    )(at_hand(received.reshape(3 * RANGES, LANES)))
    parts = lax.all_to_all(parts, AXES, 0, 0, tiled=True)
    others = [lax.ppermute(curves, "grp", [(i, (i + k) % 4) for i in range(4)]) for k in (1, 2, 3)]
    tpr, precision = pl.pallas_call(
        join_kernel,
        out_shape=(f32(4, ROWS, LANES), f32(4, ROWS, LANES)),
        in_specs=[vmem()] * 4,
        out_specs=(vmem(), vmem()),
        name="join",
    )(at_hand(curves), *[at_hand(x) for x in others])
    size = 4 * ROWS * LANES

    def again(state):
        nothing = (state[0] < 0.0).astype(jnp.int32)
        tpr, precision, roc, prc = general(bucket + nothing, label + nothing, group + nothing, group_weight)
        fix = jnp.where(jnp.arange(LANES)[None, :] == 0, roc, prc)
        return jnp.zeros((), jnp.float32), jnp.broadcast_to(fix, (8, LANES)), tpr, precision

    _, fix, tpr, precision = lax.while_loop(
        lambda state: state[0] > 0.0, again,
        (flag.reshape(()), fix, tpr.reshape(size), precision.reshape(size)))
    roc, prc = pl.pallas_call(
        area_kernel,
        out_shape=(f32(1), f32(1)),
        in_specs=[vmem(), pl.BlockSpec(memory_space=pl.ANY)],
        out_specs=(smem(), smem()),
        scratch_shapes=[pltpu.VMEM((8, LANES), jnp.float32), pltpu.SemaphoreType.DMA],
        name="area",
    )(at_hand(parts), fix)
    return tpr, precision, roc.reshape(()), prc.reshape(())


def solution(mesh):
    placed = (P(AXES), P(AXES), P(AXES), P())
    return jax.shard_map(
        on_device,
        mesh=mesh,
        in_specs=placed,
        out_specs=(P("shard"), P("shard"), P(), P()),
        check_vma=False,
    )
```

```python
import jax
import jax.numpy as jnp
from jax import lax
from jax.experimental import pallas as pl
from jax.experimental.pallas import tpu as pltpu
from jax.sharding import PartitionSpec as P


LO = 256
BLOCK = 1024
HI = 4096
BATCH = 6
CHUNK = 12

AXES = ("grp", "shard")
LANES = 128
RANGES = 128
RANGE_BITS = 13
ROWS = 64
CAP = 126
NT = (((1,), (1,)), ((), ()))
NN = (((1,), (0,)), ((), ()))
HIGHEST = lax.Precision.HIGHEST


def over_grp(x):
    every = lax.all_gather(x.reshape(x.size), "grp", axis=0, tiled=True)
    return jnp.sum(every.reshape(lax.axis_size("grp"), *x.shape), axis=0)


def histogram(bucket, label, group, group_weight, start, count):
    choose = group[:, None] == jnp.arange(group_weight.shape[0])[None, :]
    weight = jnp.sum(jnp.where(choose, group_weight[None, :], 0.0), axis=1)
    labels = label.astype(jnp.float32)
    positive = (weight * labels).astype(jnp.bfloat16)
    negative = (weight * (1.0 - labels)).astype(jnp.bfloat16)
    rows = bucket.shape[0]
    width = BLOCK
    blocks = rows // width

    def accumulate(total, items):
        ids, plus, minus = items
        high = ids // LO
        low = ids % LO
        high_one = high[:, None] == start + jnp.arange(count)[None, :]
        zero = jnp.zeros((), jnp.bfloat16)
        left = jnp.stack(
            [jnp.where(high_one, plus[:, None], zero), jnp.where(high_one, minus[:, None], zero)],
            axis=2,
        )
        left = left.reshape(width, count * 2)
        low_one = (low[:, None] == jnp.arange(LO)[None, :]).astype(jnp.bfloat16)
        product = lax.dot_general(
            left, low_one, (((0,), (0,)), ((), ())), preferred_element_type=jnp.float32
        )
        return (total + product, None)

    initial = jnp.zeros((count * 2, LO), jnp.float32)
    items = (
        bucket.reshape(blocks, width),
        positive.reshape(blocks, width),
        negative.reshape(blocks, width),
    )
    total, _ = lax.scan(accumulate, initial, items)
    return total.reshape(count, 2, LO)


def general(bucket, label, group, group_weight):
    shards = lax.axis_size("shard")
    own_rows = HI // shards
    first_row = lax.axis_index("shard") * own_rows
    ids = lax.all_gather(bucket, "shard", axis=0, tiled=True)
    clicks = lax.all_gather(label, "shard", axis=0, tiled=True)
    groups = lax.all_gather(group, "shard", axis=0, tiled=True)
    owned = histogram(ids, clicks, groups, group_weight, first_row, own_rows)
    owned = jnp.concatenate([over_grp(owned[:own_rows // 2]), over_grp(owned[own_rows // 2:])], axis=0)
    upper = (jnp.arange(LO)[:, None] >= jnp.arange(LO)[None, :]).astype(jnp.float32)
    row_suffix = jnp.dot(owned.reshape(own_rows * 2, LO), upper, precision=HIGHEST)
    row_totals = jnp.sum(owned, axis=2)
    strict = (jnp.arange(own_rows)[None, :] > jnp.arange(own_rows)[:, None]).astype(jnp.float32)
    after = jnp.dot(strict, row_totals, precision=HIGHEST)
    range_total = jnp.sum(row_totals, axis=0)
    every = lax.all_gather(range_total, "shard")
    later = jnp.arange(shards) > lax.axis_index("shard")
    higher = jnp.sum(jnp.where(later[:, None], every, 0.0), axis=0)
    overall = jnp.sum(every, axis=0)
    cumulative = row_suffix.reshape(own_rows, 2, LO) + after[:, :, None] + higher[None, :, None]
    true_pos = cumulative[:, 0, :]
    false_pos = cumulative[:, 1, :]
    pos_hist = owned[:, 0, :]
    neg_hist = owned[:, 1, :]
    tpr_curve = (true_pos / overall[0]).reshape(own_rows * LO)
    precision = true_pos / jnp.maximum(true_pos + false_pos, 1.0)
    roc_part = jnp.sum(neg_hist * (2.0 * true_pos - pos_hist))
    prc_part = jnp.sum(pos_hist * precision)
    roc_sum, prc_sum = lax.psum((roc_part, prc_part), "shard")
    auroc = roc_sum / (2.0 * overall[0] * overall[1])
    auprc = prc_sum / overall[0]
    return (tpr_curve, precision.reshape(own_rows * LO), auroc, auprc)


def iota(shape, dim):
    return lax.broadcasted_iota(jnp.int32, shape, dim)


def bf16_rows(row):
    return jnp.broadcast_to(row, (16, row.shape[1])).astype(jnp.bfloat16)


def one_hot(row, groups, value, none):
    first = iota((16, LANES), 0).astype(jnp.float32).astype(jnp.bfloat16)
    return [jnp.where(first + jnp.bfloat16(16 * k) == row, value, none) for k in range(groups)]


def route_kernel(weights_ref, bucket_ref, label_ref, group_ref, out_ref,
                 peer_s, high_s, low_s, sign_s):
    blocks = bucket_ref.shape[0]
    bucket = bucket_ref[...]
    group = group_ref[...]
    weight = jnp.zeros(group.shape, jnp.float32)
    for k in range(weights_ref.shape[0]):
        weight = jnp.where(group == k, weights_ref[k], weight)
    labels = label_ref[...].astype(jnp.float32)
    positive = (weight * labels).astype(jnp.bfloat16).astype(jnp.float32)
    negative = (weight * (1.0 - labels)).astype(jnp.bfloat16).astype(jnp.float32)
    sign_s[...] = positive - negative
    which = bucket >> RANGE_BITS
    peer = ((which & 3) << 5) | (which >> 2)
    peer_s[...] = peer.astype(jnp.float32)
    high_s[...] = ((bucket >> 7) & (ROWS - 1)).astype(jnp.float32)
    low_s[...] = (bucket & (LANES - 1)).astype(jnp.float32)

    wide = 2 * LANES
    upto = (iota((wide, wide), 0) <= iota((wide, wide), 1)).astype(jnp.bfloat16)
    none = jnp.zeros((16, LANES), jnp.bfloat16)
    unit = jnp.ones((16, LANES), jnp.bfloat16)

    first = iota((16, LANES), 0).astype(jnp.float32).astype(jnp.bfloat16)
    ones = []
    for j in range(blocks):
        row = bf16_rows(peer_s[pl.ds(j, 1), :])
        ones.append(jnp.concatenate(one_hot(row, 8, unit, none), axis=0))
    pairs = [jnp.concatenate(ones[j:j + 2], axis=1) for j in range(0, blocks, 2)]
    count = jnp.zeros((RANGES, LANES), jnp.float32)
    left = []
    right = []
    for v in range(0, len(pairs), BATCH):
        batch = pairs[v:v + BATCH]
        seen_all = lax.dot_general(jnp.concatenate(batch, axis=0), upto, NN, preferred_element_type=jnp.float32)
        for w in range(len(batch)):
            seen = seen_all[w * RANGES:(w + 1) * RANGES]
            capped = jnp.minimum(count, 256.0).astype(jnp.bfloat16)
            for h in range(2):
                j = 2 * (v + w) + h
                before = ones[j] * (seen[:, h * LANES:(h + 1) * LANES].astype(jnp.bfloat16) + capped)
                rank = before[:16]
                for k in range(16, RANGES, 16):
                    rank = rank + before[k:k + 16]
                rank = jnp.sum(rank.astype(jnp.float32), axis=0, keepdims=True) - 1.0
                upper = rank >= LANES // 2
                rank = bf16_rows(jnp.where(upper, rank - LANES // 2, rank))
                upper = bf16_rows(jnp.where(upper, 1.0, 0.0)) > none
                high = bf16_rows(high_s[pl.ds(j, 1), :])
                low = bf16_rows(low_s[pl.ds(j, 1), :])
                sign = bf16_rows(sign_s[pl.ds(j, 1), :])
                same = [first + jnp.bfloat16(16 * k) == rank for k in range(4)]
                left.append(jnp.concatenate(
                    [jnp.where(m, value, none) for value in (high, low, sign) for m in same], axis=0))
                parts = [ones[j][16 * k:16 * k + 16] for k in range(8)]
                right.append(jnp.concatenate(
                    [jnp.where(upper, none, part) for part in parts] + [jnp.where(upper, part, none) for part in parts],
                    axis=0))
            count = count + jnp.broadcast_to(seen[:, wide - 1:wide], (RANGES, LANES))
    placed = jnp.zeros((3 * LANES // 2, 2 * RANGES), jnp.float32)
    for v in range(0, blocks, CHUNK):
        placed = placed + lax.dot_general(
            jnp.concatenate(left[v:v + CHUNK], axis=1), jnp.concatenate(right[v:v + CHUNK], axis=1), NT,
            preferred_element_type=jnp.float32)

    def slots(c):
        rows = placed[c * LANES // 2:(c + 1) * LANES // 2]
        return jnp.concatenate([rows[:, :RANGES], rows[:, RANGES:]], axis=0)

    full = jnp.max(jnp.where(count > CAP, 1.0, 0.0), axis=0, keepdims=True)
    full = jnp.max(full, axis=1, keepdims=True)

    slot = iota((LANES, RANGES), 0)
    real = slot < CAP
    high = slots(0)
    low = slots(1)
    sign = jnp.where(real, slots(2), 0.0)
    pos = jnp.maximum(sign, 0.0)
    neg = jnp.maximum(-sign, 0.0)
    p0 = iota((RANGES, RANGES), 0)
    p1 = iota((RANGES, RANGES), 1)
    r0 = ((p0 & 31) << 2) | (p0 >> 5)
    r1 = ((p1 & 31) << 2) | (p1 >> 5)
    above = (r0 > r1).astype(jnp.bfloat16)
    both = jnp.concatenate([pos, neg], axis=0).astype(jnp.bfloat16)
    later = lax.dot_general(both, above, NN, preferred_element_type=jnp.float32)
    for c, own in ((1, pos), (2, neg)):
        higher = jnp.sum(later[(c - 1) * LANES:c * LANES], axis=0, keepdims=True)
        total = jnp.sum(jnp.sum(own, axis=0, keepdims=True), axis=1, keepdims=True)
        sent = jnp.where(real, own, jnp.where(slot == CAP, higher, total))
        out_ref[pl.ds(c, RANGES, stride=3), :] = sent.T
    out_ref[pl.ds(0, RANGES, stride=3), :] = jnp.where(real, LANES * high + low, full).T


def in_three(x):
    first = x.astype(jnp.bfloat16)
    rest = x - first.astype(jnp.float32)
    second = rest.astype(jnp.bfloat16)
    rest = rest - second.astype(jnp.float32)
    return first, second, rest.astype(jnp.bfloat16)


def curve_kernel(in_ref, curve_ref, part_ref, fix_ref, flag_ref):
    none = jnp.zeros((16, LANES), jnp.bfloat16)
    unit = jnp.ones((16, LANES), jnp.bfloat16)
    first = iota((16, LANES), 0).astype(jnp.float32).astype(jnp.bfloat16)
    real = iota((16, LANES), 1) < CAP
    left = []
    right = []
    for q in range(RANGES):
        place = in_ref[pl.ds(3 * q, 1), :]
        high = jnp.floor(place * (1.0 / LANES))
        low = bf16_rows(place - LANES * high)
        high = bf16_rows(high)
        pos = jnp.where(real, jnp.broadcast_to(in_ref[pl.ds(3 * q + 1, 1), :], (16, LANES)), 0.0).astype(jnp.bfloat16)
        neg = jnp.where(real, jnp.broadcast_to(in_ref[pl.ds(3 * q + 2, 1), :], (16, LANES)), 0.0).astype(jnp.bfloat16)
        same = [first + jnp.bfloat16(16 * k) == high for k in range(4)]
        left.append(jnp.concatenate(
            [jnp.where(m, pos, none) for m in same] + [jnp.where(m, neg, none) for m in same], axis=0))
        right.append(jnp.concatenate(one_hot(low, 8, unit, none), axis=0))
    hist = lax.dot_general(jnp.concatenate(left, axis=1), jnp.concatenate(right, axis=1), NT,
                           preferred_element_type=jnp.float32)
    sums = in_ref[pl.ds(0, 24), :]
    for q in range(24, 3 * RANGES, 24):
        sums = sums + in_ref[pl.ds(q, 24), :]
    kind = iota((24, LANES), 0) % 3
    sums = [jnp.sum(jnp.where(kind == c, sums, 0.0), axis=0, keepdims=True) for c in range(3)]
    flag = sums[0][:, CAP:CAP + 1]
    higher_pos = sums[1][:, CAP:CAP + 1]
    total_pos = sums[1][:, CAP + 1:CAP + 2]
    higher_neg = sums[2][:, CAP:CAP + 1]
    total_neg = sums[2][:, CAP + 1:CAP + 2]
    roc_scale = 1.0 / (2.0 * total_pos * total_neg)
    prc_scale = 1.0 / total_pos
    upper = (iota((LANES, LANES), 0) >= iota((LANES, LANES), 1)).astype(jnp.bfloat16)
    row = iota((2 * ROWS, 2 * ROWS), 0)
    col = iota((2 * ROWS, 2 * ROWS), 1)
    below = ((col > row) & ((col >= ROWS) == (row >= ROWS))).astype(jnp.bfloat16)
    pieces = in_three(hist)
    in_row = lax.dot_general(jnp.concatenate(pieces, axis=1), jnp.concatenate([upper] * 3, axis=0), NN,
                             preferred_element_type=jnp.float32)
    rows_after = lax.dot_general(jnp.concatenate([below] * 3, axis=1), jnp.concatenate(pieces, axis=0), NN,
                                 preferred_element_type=jnp.float32)
    cumulative = in_row + jnp.sum(rows_after, axis=1, keepdims=True)
    true_pos = cumulative[:ROWS] + higher_pos
    false_pos = cumulative[ROWS:] + higher_neg
    pos_hist = hist[:ROWS]
    neg_hist = hist[ROWS:]
    precision = true_pos / jnp.maximum(true_pos + false_pos, 1.0)
    curve_ref[0] = true_pos / total_pos
    curve_ref[1] = precision
    roc = jnp.sum(neg_hist * (2.0 * true_pos - pos_hist), axis=0, keepdims=True)
    prc = jnp.sum(pos_hist * precision, axis=0, keepdims=True)
    roc = jnp.sum(roc, axis=1, keepdims=True) * roc_scale
    prc = jnp.sum(prc, axis=1, keepdims=True) * prc_scale
    lane = iota((RANGES, 1, LANES), 2)
    part_ref[...] = jnp.where(lane == 0, roc[None], jnp.where(lane == 1, prc[None], flag[None]))
    fix_ref[...] = jnp.zeros((8, LANES), jnp.float32)
    flag_ref[0] = jnp.max(flag)


def join_kernel(own_ref, one_ref, two_ref, three_ref, tpr_ref, precision_ref):
    me = lax.axis_index("grp")
    for k, ref in enumerate((own_ref, one_ref, two_ref, three_ref)):
        source = (me - k) & 3
        tpr_ref[source] = ref[0]
        precision_ref[source] = ref[1]


def area_kernel(part_ref, fix_ref, roc_ref, prc_ref, fix_s, done):
    sums = jnp.sum(part_ref[...].reshape(RANGES, LANES), axis=0, keepdims=True)
    lane = iota((1, LANES), 1)
    roc_ref[0] = jnp.sum(jnp.where(lane == 0, sums, 0.0))
    prc_ref[0] = jnp.sum(jnp.where(lane == 1, sums, 0.0))

    @pl.when(jnp.sum(jnp.where(lane == 2, sums, 0.0)) > 0.0)
    def _():
        copy = pltpu.make_async_copy(fix_ref, fix_s, done)
        copy.start()
        copy.wait()
        fix = fix_s[0:1, :]
        roc_ref[0] = jnp.sum(jnp.where(lane == 0, fix, 0.0))
        prc_ref[0] = jnp.sum(jnp.where(lane == 1, fix, 0.0))


def vmem():
    return pl.BlockSpec(memory_space=pltpu.VMEM)


def smem():
    return pl.BlockSpec(memory_space=pltpu.SMEM)


def f32(*shape):
    return jax.ShapeDtypeStruct(shape, jnp.float32)


def near(*shape):
    return pltpu.VMEM(shape, jnp.float32)


def at_hand(x):
    return pltpu.with_memory_space_constraint(x, pltpu.VMEM)


def on_device(bucket, label, group, group_weight):
    blocks = bucket.shape[0] // LANES
    message = pl.pallas_call(
        route_kernel,
        out_shape=near(3 * RANGES, LANES),
        in_specs=[smem(), vmem(), vmem(), vmem()],
        out_specs=vmem(),
        scratch_shapes=[pltpu.VMEM((blocks, LANES), jnp.float32)] * 4,
        name="route",
    )(group_weight, bucket.reshape(blocks, LANES), label.reshape(blocks, LANES), group.reshape(blocks, LANES))
    received = lax.all_to_all(message.reshape(RANGES, 1, 3 * LANES), AXES, 0, 0, tiled=True)
    curves, parts, fix, flag = pl.pallas_call(
        curve_kernel,
        out_shape=(near(2, ROWS, LANES), near(RANGES, 1, LANES), f32(8, LANES), f32(1)),
        in_specs=[vmem()],
        out_specs=(vmem(), vmem(), vmem(), smem()),
        name="curve",
    )(at_hand(received.reshape(3 * RANGES, LANES)))
    parts = lax.all_to_all(parts, AXES, 0, 0, tiled=True)
    others = [lax.ppermute(curves, "grp", [(i, (i + k) % 4) for i in range(4)]) for k in (1, 2, 3)]
    tpr, precision = pl.pallas_call(
        join_kernel,
        out_shape=(f32(4, ROWS, LANES), f32(4, ROWS, LANES)),
        in_specs=[vmem()] * 4,
        out_specs=(vmem(), vmem()),
        name="join",
    )(at_hand(curves), *[at_hand(x) for x in others])
    size = 4 * ROWS * LANES

    def again(state):
        nothing = (state[0] < 0.0).astype(jnp.int32)
        tpr, precision, roc, prc = general(bucket + nothing, label + nothing, group + nothing, group_weight)
        fix = jnp.where(jnp.arange(LANES)[None, :] == 0, roc, prc)
        return jnp.zeros((), jnp.float32), jnp.broadcast_to(fix, (8, LANES)), tpr, precision

    _, fix, tpr, precision = lax.while_loop(
        lambda state: state[0] > 0.0, again,
        (flag.reshape(()), fix, tpr.reshape(size), precision.reshape(size)))
    roc, prc = pl.pallas_call(
        area_kernel,
        out_shape=(f32(1), f32(1)),
        in_specs=[vmem(), pl.BlockSpec(memory_space=pl.ANY)],
        out_specs=(smem(), smem()),
        scratch_shapes=[pltpu.VMEM((8, LANES), jnp.float32), pltpu.SemaphoreType.DMA],
        name="area",
    )(at_hand(parts), fix)
    return tpr, precision, roc.reshape(()), prc.reshape(())


def solution(mesh):
    placed = (P(AXES), P(AXES), P(AXES), P())
    return jax.shard_map(
        on_device,
        mesh=mesh,
        in_specs=placed,
        out_specs=(P("shard"), P("shard"), P(), P()),
        check_vma=False,
    )
```

```python
import jax
import jax.numpy as jnp
from jax import lax
from jax.experimental import pallas as pl
from jax.experimental.pallas import tpu as pltpu
from jax.sharding import PartitionSpec as P


LO = 256
BLOCK = 1024
HI = 4096
BATCH = 6
CHUNK = 12

AXES = ("grp", "shard")
LANES = 128
RANGES = 128
RANGE_BITS = 13
ROWS = 64
CAP = 126
NT = (((1,), (1,)), ((), ()))
NN = (((1,), (0,)), ((), ()))
HIGHEST = lax.Precision.HIGHEST


def over_grp(x):
    every = lax.all_gather(x.reshape(x.size), "grp", axis=0, tiled=True)
    return jnp.sum(every.reshape(lax.axis_size("grp"), *x.shape), axis=0)


def histogram(bucket, label, group, group_weight, start, count):
    choose = group[:, None] == jnp.arange(group_weight.shape[0])[None, :]
    weight = jnp.sum(jnp.where(choose, group_weight[None, :], 0.0), axis=1)
    labels = label.astype(jnp.float32)
    positive = (weight * labels).astype(jnp.bfloat16)
    negative = (weight * (1.0 - labels)).astype(jnp.bfloat16)
    rows = bucket.shape[0]
    width = BLOCK
    blocks = rows // width

    def accumulate(total, items):
        ids, plus, minus = items
        high = ids // LO
        low = ids % LO
        high_one = high[:, None] == start + jnp.arange(count)[None, :]
        zero = jnp.zeros((), jnp.bfloat16)
        left = jnp.stack(
            [jnp.where(high_one, plus[:, None], zero), jnp.where(high_one, minus[:, None], zero)],
            axis=2,
        )
        left = left.reshape(width, count * 2)
        low_one = (low[:, None] == jnp.arange(LO)[None, :]).astype(jnp.bfloat16)
        product = lax.dot_general(
            left, low_one, (((0,), (0,)), ((), ())), preferred_element_type=jnp.float32
        )
        return (total + product, None)

    initial = jnp.zeros((count * 2, LO), jnp.float32)
    items = (
        bucket.reshape(blocks, width),
        positive.reshape(blocks, width),
        negative.reshape(blocks, width),
    )
    total, _ = lax.scan(accumulate, initial, items)
    return total.reshape(count, 2, LO)


def general(bucket, label, group, group_weight):
    shards = lax.axis_size("shard")
    own_rows = HI // shards
    first_row = lax.axis_index("shard") * own_rows
    ids = lax.all_gather(bucket, "shard", axis=0, tiled=True)
    clicks = lax.all_gather(label, "shard", axis=0, tiled=True)
    groups = lax.all_gather(group, "shard", axis=0, tiled=True)
    owned = histogram(ids, clicks, groups, group_weight, first_row, own_rows)
    owned = jnp.concatenate([over_grp(owned[:own_rows // 2]), over_grp(owned[own_rows // 2:])], axis=0)
    upper = (jnp.arange(LO)[:, None] >= jnp.arange(LO)[None, :]).astype(jnp.float32)
    row_suffix = jnp.dot(owned.reshape(own_rows * 2, LO), upper, precision=HIGHEST)
    row_totals = jnp.sum(owned, axis=2)
    strict = (jnp.arange(own_rows)[None, :] > jnp.arange(own_rows)[:, None]).astype(jnp.float32)
    after = jnp.dot(strict, row_totals, precision=HIGHEST)
    range_total = jnp.sum(row_totals, axis=0)
    every = lax.all_gather(range_total, "shard")
    later = jnp.arange(shards) > lax.axis_index("shard")
    higher = jnp.sum(jnp.where(later[:, None], every, 0.0), axis=0)
    overall = jnp.sum(every, axis=0)
    cumulative = row_suffix.reshape(own_rows, 2, LO) + after[:, :, None] + higher[None, :, None]
    true_pos = cumulative[:, 0, :]
    false_pos = cumulative[:, 1, :]
    pos_hist = owned[:, 0, :]
    neg_hist = owned[:, 1, :]
    tpr_curve = (true_pos / overall[0]).reshape(own_rows * LO)
    precision = true_pos / jnp.maximum(true_pos + false_pos, 1.0)
    roc_part = jnp.sum(neg_hist * (2.0 * true_pos - pos_hist))
    prc_part = jnp.sum(pos_hist * precision)
    roc_sum, prc_sum = lax.psum((roc_part, prc_part), "shard")
    auroc = roc_sum / (2.0 * overall[0] * overall[1])
    auprc = prc_sum / overall[0]
    return (tpr_curve, precision.reshape(own_rows * LO), auroc, auprc)


def iota(shape, dim):
    return lax.broadcasted_iota(jnp.int32, shape, dim)


def bf16_rows(row):
    return jnp.broadcast_to(row, (16, row.shape[1])).astype(jnp.bfloat16)


def one_hot(row, groups, value, none):
    first = iota((16, LANES), 0).astype(jnp.float32).astype(jnp.bfloat16)
    return [jnp.where(first + jnp.bfloat16(16 * k) == row, value, none) for k in range(groups)]


def route_kernel(weights_ref, bucket_ref, label_ref, group_ref, out_ref,
                 peer_s, high_s, low_s, sign_s):
    blocks = bucket_ref.shape[0]
    bucket = bucket_ref[...]
    group = group_ref[...]
    weight = jnp.zeros(group.shape, jnp.float32)
    for k in range(weights_ref.shape[0]):
        weight = jnp.where(group == k, weights_ref[k], weight)
    labels = label_ref[...].astype(jnp.float32)
    positive = (weight * labels).astype(jnp.bfloat16).astype(jnp.float32)
    negative = (weight * (1.0 - labels)).astype(jnp.bfloat16).astype(jnp.float32)
    sign_s[...] = positive - negative
    which = bucket >> RANGE_BITS
    peer = ((which & 3) << 5) | (which >> 2)
    peer_s[...] = peer.astype(jnp.float32)
    high_s[...] = ((bucket >> 7) & (ROWS - 1)).astype(jnp.float32)
    low_s[...] = (bucket & (LANES - 1)).astype(jnp.float32)

    wide = 2 * LANES
    upto = (iota((wide, wide), 0) <= iota((wide, wide), 1)).astype(jnp.bfloat16)
    none = jnp.zeros((16, LANES), jnp.bfloat16)
    unit = jnp.ones((16, LANES), jnp.bfloat16)

    first = iota((16, LANES), 0).astype(jnp.float32).astype(jnp.bfloat16)
    ones = []
    for j in range(blocks):
        row = bf16_rows(peer_s[pl.ds(j, 1), :])
        ones.append(jnp.concatenate(one_hot(row, 8, unit, none), axis=0))
    pairs = [jnp.concatenate(ones[j:j + 2], axis=1) for j in range(0, blocks, 2)]
    count = jnp.zeros((RANGES, LANES), jnp.float32)
    left = []
    right = []
    for v in range(0, len(pairs), BATCH):
        batch = pairs[v:v + BATCH]
        seen_all = lax.dot_general(jnp.concatenate(batch, axis=0), upto, NN, preferred_element_type=jnp.float32)
        for w in range(len(batch)):
            seen = seen_all[w * RANGES:(w + 1) * RANGES]
            for h in range(2):
                j = 2 * (v + w) + h
                mine = ones[j].astype(jnp.float32)
                before = seen[:, h * LANES:(h + 1) * LANES] + count
                rank = jnp.sum(mine * before, axis=0, keepdims=True) - 1.0
                upper = rank >= LANES // 2
                rank = bf16_rows(jnp.where(upper, rank - LANES // 2, rank))
                upper = bf16_rows(jnp.where(upper, 1.0, 0.0)) > none
                high = bf16_rows(high_s[pl.ds(j, 1), :])
                low = bf16_rows(low_s[pl.ds(j, 1), :])
                sign = bf16_rows(sign_s[pl.ds(j, 1), :])
                same = [first + jnp.bfloat16(16 * k) == rank for k in range(4)]
                left.append(jnp.concatenate(
                    [jnp.where(m, value, none) for value in (high, low, sign) for m in same], axis=0))
                parts = [ones[j][16 * k:16 * k + 16] for k in range(8)]
                right.append(jnp.concatenate(
                    [jnp.where(upper, none, part) for part in parts] + [jnp.where(upper, part, none) for part in parts],
                    axis=0))
            count = count + jnp.broadcast_to(seen[:, wide - 1:wide], (RANGES, LANES))
    placed = jnp.zeros((3 * LANES // 2, 2 * RANGES), jnp.float32)
    for v in range(0, blocks, CHUNK):
        placed = placed + lax.dot_general(
            jnp.concatenate(left[v:v + CHUNK], axis=1), jnp.concatenate(right[v:v + CHUNK], axis=1), NT,
            preferred_element_type=jnp.float32)

    def slots(c):
        rows = placed[c * LANES // 2:(c + 1) * LANES // 2]
        return jnp.concatenate([rows[:, :RANGES], rows[:, RANGES:]], axis=0)

    full = jnp.max(jnp.where(count > CAP, 1.0, 0.0), axis=0, keepdims=True)
    full = jnp.max(full, axis=1, keepdims=True)

    slot = iota((LANES, RANGES), 0)
    real = slot < CAP
    high = slots(0)
    low = slots(1)
    sign = jnp.where(real, slots(2), 0.0)
    pos = jnp.maximum(sign, 0.0)
    neg = jnp.maximum(-sign, 0.0)
    p0 = iota((RANGES, RANGES), 0)
    p1 = iota((RANGES, RANGES), 1)
    r0 = ((p0 & 31) << 2) | (p0 >> 5)
    r1 = ((p1 & 31) << 2) | (p1 >> 5)
    above = (r0 > r1).astype(jnp.bfloat16)
    both = jnp.concatenate([pos, neg], axis=0).astype(jnp.bfloat16)
    later = lax.dot_general(both, above, NN, preferred_element_type=jnp.float32)
    for c, own in ((1, pos), (2, neg)):
        higher = jnp.sum(later[(c - 1) * LANES:c * LANES], axis=0, keepdims=True)
        total = jnp.sum(jnp.sum(own, axis=0, keepdims=True), axis=1, keepdims=True)
        sent = jnp.where(real, own, jnp.where(slot == CAP, higher, total))
        out_ref[pl.ds(c, RANGES, stride=3), :] = sent.T
    out_ref[pl.ds(0, RANGES, stride=3), :] = jnp.where(real, LANES * high + low, full).T


def in_three(x):
    first = x.astype(jnp.bfloat16)
    rest = x - first.astype(jnp.float32)
    second = rest.astype(jnp.bfloat16)
    rest = rest - second.astype(jnp.float32)
    return first, second, rest.astype(jnp.bfloat16)


def curve_kernel(in_ref, curve_ref, part_ref, note_ref):
    none = jnp.zeros((16, LANES), jnp.bfloat16)
    unit = jnp.ones((16, LANES), jnp.bfloat16)
    first = iota((16, LANES), 0).astype(jnp.float32).astype(jnp.bfloat16)
    real = iota((16, LANES), 1) < CAP
    left = []
    right = []
    for q in range(RANGES):
        place = in_ref[pl.ds(3 * q, 1), :]
        high = jnp.floor(place * (1.0 / LANES))
        low = bf16_rows(place - LANES * high)
        high = bf16_rows(high)
        pos = jnp.where(real, jnp.broadcast_to(in_ref[pl.ds(3 * q + 1, 1), :], (16, LANES)), 0.0).astype(jnp.bfloat16)
        neg = jnp.where(real, jnp.broadcast_to(in_ref[pl.ds(3 * q + 2, 1), :], (16, LANES)), 0.0).astype(jnp.bfloat16)
        same = [first + jnp.bfloat16(16 * k) == high for k in range(4)]
        left.append(jnp.concatenate(
            [jnp.where(m, pos, none) for m in same] + [jnp.where(m, neg, none) for m in same], axis=0))
        right.append(jnp.concatenate(one_hot(low, 8, unit, none), axis=0))
    hist = lax.dot_general(jnp.concatenate(left, axis=1), jnp.concatenate(right, axis=1), NT,
                           preferred_element_type=jnp.float32)
    sums = in_ref[pl.ds(0, 24), :]
    for q in range(24, 3 * RANGES, 24):
        sums = sums + in_ref[pl.ds(q, 24), :]
    kind = iota((24, LANES), 0) % 3
    sums = [jnp.sum(jnp.where(kind == c, sums, 0.0), axis=0, keepdims=True) for c in range(3)]
    flag = sums[0][:, CAP:CAP + 1]
    higher_pos = sums[1][:, CAP:CAP + 1]
    total_pos = sums[1][:, CAP + 1:CAP + 2]
    higher_neg = sums[2][:, CAP:CAP + 1]
    total_neg = sums[2][:, CAP + 1:CAP + 2]
    upper = (iota((LANES, LANES), 0) >= iota((LANES, LANES), 1)).astype(jnp.bfloat16)
    row = iota((2 * ROWS, 2 * ROWS), 0)
    col = iota((2 * ROWS, 2 * ROWS), 1)
    below = ((col > row) & ((col >= ROWS) == (row >= ROWS))).astype(jnp.bfloat16)
    pieces = in_three(hist)
    in_row = lax.dot_general(jnp.concatenate(pieces, axis=1), jnp.concatenate([upper] * 3, axis=0), NN,
                             preferred_element_type=jnp.float32)
    rows_after = lax.dot_general(jnp.concatenate([below] * 3, axis=1), jnp.concatenate(pieces, axis=0), NN,
                                 preferred_element_type=jnp.float32)
    cumulative = in_row + jnp.sum(rows_after, axis=1, keepdims=True)
    true_pos = cumulative[:ROWS] + higher_pos
    false_pos = cumulative[ROWS:] + higher_neg
    pos_hist = hist[:ROWS]
    neg_hist = hist[ROWS:]
    precision = true_pos / jnp.maximum(true_pos + false_pos, 1.0)
    curve_ref[0] = true_pos / total_pos
    curve_ref[1] = precision
    roc = jnp.sum(neg_hist * (2.0 * true_pos - pos_hist), axis=0, keepdims=True)
    prc = jnp.sum(pos_hist * precision, axis=0, keepdims=True)
    roc = jnp.sum(roc, axis=1, keepdims=True) / (2.0 * total_pos * total_neg)
    prc = jnp.sum(prc, axis=1, keepdims=True) / total_pos
    lane = iota((RANGES, 1, LANES), 2)
    part_ref[...] = jnp.where(lane == 0, roc[None], jnp.where(lane == 1, prc[None], flag[None]))
    note_ref[...] = jnp.broadcast_to(flag, (8, LANES))


def join_kernel(own_ref, one_ref, two_ref, three_ref, note_ref, tpr_ref, precision_ref, fix_ref, flag_ref):
    fix_ref[...] = jnp.zeros((8, LANES), jnp.float32)
    flag_ref[0] = jnp.max(note_ref[...])
    me = lax.axis_index("grp")
    for k, ref in enumerate((own_ref, one_ref, two_ref, three_ref)):
        source = (me - k) & 3
        tpr_ref[source] = ref[0]
        precision_ref[source] = ref[1]


def area_kernel(part_ref, fix_ref, roc_ref, prc_ref, fix_s, done):
    sums = jnp.sum(part_ref[...].reshape(RANGES, LANES), axis=0, keepdims=True)
    lane = iota((1, LANES), 1)
    roc_ref[0] = jnp.sum(jnp.where(lane == 0, sums, 0.0))
    prc_ref[0] = jnp.sum(jnp.where(lane == 1, sums, 0.0))

    @pl.when(jnp.sum(jnp.where(lane == 2, sums, 0.0)) > 0.0)
    def _():
        copy = pltpu.make_async_copy(fix_ref, fix_s, done)
        copy.start()
        copy.wait()
        fix = fix_s[0:1, :]
        roc_ref[0] = jnp.sum(jnp.where(lane == 0, fix, 0.0))
        prc_ref[0] = jnp.sum(jnp.where(lane == 1, fix, 0.0))


def vmem():
    return pl.BlockSpec(memory_space=pltpu.VMEM)


def smem():
    return pl.BlockSpec(memory_space=pltpu.SMEM)


def f32(*shape):
    return jax.ShapeDtypeStruct(shape, jnp.float32)


def near(*shape):
    return pltpu.VMEM(shape, jnp.float32)


def at_hand(x):
    return pltpu.with_memory_space_constraint(x, pltpu.VMEM)


def on_device(bucket, label, group, group_weight):
    blocks = bucket.shape[0] // LANES
    message = pl.pallas_call(
        route_kernel,
        out_shape=near(3 * RANGES, LANES),
        in_specs=[smem(), vmem(), vmem(), vmem()],
        out_specs=vmem(),
        scratch_shapes=[pltpu.VMEM((blocks, LANES), jnp.float32)] * 4,
        name="route",
    )(group_weight, bucket.reshape(blocks, LANES), label.reshape(blocks, LANES), group.reshape(blocks, LANES))
    received = lax.all_to_all(message.reshape(RANGES, 1, 3 * LANES), AXES, 0, 0, tiled=True)
    curves, parts, note = pl.pallas_call(
        curve_kernel,
        out_shape=(near(2, ROWS, LANES), near(RANGES, 1, LANES), near(8, LANES)),
        in_specs=[vmem()],
        out_specs=(vmem(), vmem(), vmem()),
        name="curve",
    )(at_hand(received.reshape(3 * RANGES, LANES)))
    parts = lax.all_to_all(parts, AXES, 0, 0, tiled=True)
    others = [lax.ppermute(curves, "grp", [(i, (i + k) % 4) for i in range(4)]) for k in (1, 2, 3)]
    tpr, precision, fix, flag = pl.pallas_call(
        join_kernel,
        out_shape=(f32(4, ROWS, LANES), f32(4, ROWS, LANES), f32(8, LANES), f32(1)),
        in_specs=[vmem()] * 5,
        out_specs=(vmem(), vmem(), vmem(), smem()),
        name="join",
    )(at_hand(curves), *[at_hand(x) for x in others], at_hand(note))
    size = 4 * ROWS * LANES

    def again(state):
        nothing = (state[0] < 0.0).astype(jnp.int32)
        tpr, precision, roc, prc = general(bucket + nothing, label + nothing, group + nothing, group_weight)
        fix = jnp.where(jnp.arange(LANES)[None, :] == 0, roc, prc)
        return jnp.zeros((), jnp.float32), jnp.broadcast_to(fix, (8, LANES)), tpr, precision

    _, fix, tpr, precision = lax.while_loop(
        lambda state: state[0] > 0.0, again,
        (flag.reshape(()), fix, tpr.reshape(size), precision.reshape(size)))
    roc, prc = pl.pallas_call(
        area_kernel,
        out_shape=(f32(1), f32(1)),
        in_specs=[vmem(), pl.BlockSpec(memory_space=pl.ANY)],
        out_specs=(smem(), smem()),
        scratch_shapes=[pltpu.VMEM((8, LANES), jnp.float32), pltpu.SemaphoreType.DMA],
        name="area",
    )(at_hand(parts), fix)
    return tpr, precision, roc.reshape(()), prc.reshape(())


def solution(mesh):
    placed = (P(AXES), P(AXES), P(AXES), P())
    return jax.shard_map(
        on_device,
        mesh=mesh,
        in_specs=placed,
        out_specs=(P("shard"), P("shard"), P(), P()),
        check_vma=False,
    )
```

```python
import jax
import jax.numpy as jnp
from jax import lax
from jax.experimental import pallas as pl
from jax.experimental.pallas import tpu as pltpu
from jax.sharding import PartitionSpec as P


LO = 256
BLOCK = 1024
HI = 4096
BATCH = 6
CHUNK = 12

AXES = ("grp", "shard")
LANES = 128
RANGES = 128
RANGE_BITS = 13
ROWS = 64
CAP = 126
NT = (((1,), (1,)), ((), ()))
NN = (((1,), (0,)), ((), ()))
HIGHEST = lax.Precision.HIGHEST


def over_grp(x):
    every = lax.all_gather(x.reshape(x.size), "grp", axis=0, tiled=True)
    return jnp.sum(every.reshape(lax.axis_size("grp"), *x.shape), axis=0)


def histogram(bucket, label, group, group_weight, start, count):
    choose = group[:, None] == jnp.arange(group_weight.shape[0])[None, :]
    weight = jnp.sum(jnp.where(choose, group_weight[None, :], 0.0), axis=1)
    labels = label.astype(jnp.float32)
    positive = (weight * labels).astype(jnp.bfloat16)
    negative = (weight * (1.0 - labels)).astype(jnp.bfloat16)
    rows = bucket.shape[0]
    width = BLOCK
    blocks = rows // width

    def accumulate(total, items):
        ids, plus, minus = items
        high = ids // LO
        low = ids % LO
        high_one = high[:, None] == start + jnp.arange(count)[None, :]
        zero = jnp.zeros((), jnp.bfloat16)
        left = jnp.stack(
            [jnp.where(high_one, plus[:, None], zero), jnp.where(high_one, minus[:, None], zero)],
            axis=2,
        )
        left = left.reshape(width, count * 2)
        low_one = (low[:, None] == jnp.arange(LO)[None, :]).astype(jnp.bfloat16)
        product = lax.dot_general(
            left, low_one, (((0,), (0,)), ((), ())), preferred_element_type=jnp.float32
        )
        return (total + product, None)

    initial = jnp.zeros((count * 2, LO), jnp.float32)
    items = (
        bucket.reshape(blocks, width),
        positive.reshape(blocks, width),
        negative.reshape(blocks, width),
    )
    total, _ = lax.scan(accumulate, initial, items)
    return total.reshape(count, 2, LO)


def general(bucket, label, group, group_weight):
    shards = lax.axis_size("shard")
    own_rows = HI // shards
    first_row = lax.axis_index("shard") * own_rows
    ids = lax.all_gather(bucket, "shard", axis=0, tiled=True)
    clicks = lax.all_gather(label, "shard", axis=0, tiled=True)
    groups = lax.all_gather(group, "shard", axis=0, tiled=True)
    owned = histogram(ids, clicks, groups, group_weight, first_row, own_rows)
    owned = jnp.concatenate([over_grp(owned[:own_rows // 2]), over_grp(owned[own_rows // 2:])], axis=0)
    upper = (jnp.arange(LO)[:, None] >= jnp.arange(LO)[None, :]).astype(jnp.float32)
    row_suffix = jnp.dot(owned.reshape(own_rows * 2, LO), upper, precision=HIGHEST)
    row_totals = jnp.sum(owned, axis=2)
    strict = (jnp.arange(own_rows)[None, :] > jnp.arange(own_rows)[:, None]).astype(jnp.float32)
    after = jnp.dot(strict, row_totals, precision=HIGHEST)
    range_total = jnp.sum(row_totals, axis=0)
    every = lax.all_gather(range_total, "shard")
    later = jnp.arange(shards) > lax.axis_index("shard")
    higher = jnp.sum(jnp.where(later[:, None], every, 0.0), axis=0)
    overall = jnp.sum(every, axis=0)
    cumulative = row_suffix.reshape(own_rows, 2, LO) + after[:, :, None] + higher[None, :, None]
    true_pos = cumulative[:, 0, :]
    false_pos = cumulative[:, 1, :]
    pos_hist = owned[:, 0, :]
    neg_hist = owned[:, 1, :]
    tpr_curve = (true_pos / overall[0]).reshape(own_rows * LO)
    precision = true_pos / jnp.maximum(true_pos + false_pos, 1.0)
    roc_part = jnp.sum(neg_hist * (2.0 * true_pos - pos_hist))
    prc_part = jnp.sum(pos_hist * precision)
    roc_sum, prc_sum = lax.psum((roc_part, prc_part), "shard")
    auroc = roc_sum / (2.0 * overall[0] * overall[1])
    auprc = prc_sum / overall[0]
    return (tpr_curve, precision.reshape(own_rows * LO), auroc, auprc)


def iota(shape, dim):
    return lax.broadcasted_iota(jnp.int32, shape, dim)


def bf16_rows(row):
    return jnp.broadcast_to(row, (16, row.shape[1])).astype(jnp.bfloat16)


def one_hot(row, groups, value, none):
    first = iota((16, LANES), 0).astype(jnp.float32).astype(jnp.bfloat16)
    return [jnp.where(first + jnp.bfloat16(16 * k) == row, value, none) for k in range(groups)]


def route_kernel(weights_ref, bucket_ref, label_ref, group_ref, out_ref,
                 peer_s, high_s, low_s, sign_s):
    blocks = bucket_ref.shape[0]
    bucket = bucket_ref[...]
    group = group_ref[...]
    weight = jnp.zeros(group.shape, jnp.float32)
    for k in range(weights_ref.shape[0]):
        weight = jnp.where(group == k, weights_ref[k], weight)
    labels = label_ref[...].astype(jnp.float32)
    positive = (weight * labels).astype(jnp.bfloat16).astype(jnp.float32)
    negative = (weight * (1.0 - labels)).astype(jnp.bfloat16).astype(jnp.float32)
    sign_s[...] = positive - negative
    which = bucket >> RANGE_BITS
    peer = ((which & 3) << 5) | (which >> 2)
    peer_s[...] = peer.astype(jnp.float32)
    high_s[...] = ((bucket >> 7) & (ROWS - 1)).astype(jnp.float32)
    low_s[...] = (bucket & (LANES - 1)).astype(jnp.float32)

    wide = 2 * LANES
    upto = (iota((wide, wide), 0) <= iota((wide, wide), 1)).astype(jnp.bfloat16)
    none = jnp.zeros((16, LANES), jnp.bfloat16)
    unit = jnp.ones((16, LANES), jnp.bfloat16)

    first = iota((16, LANES), 0).astype(jnp.float32).astype(jnp.bfloat16)
    ones = []
    for j in range(blocks):
        row = bf16_rows(peer_s[pl.ds(j, 1), :])
        ones.append(jnp.concatenate(one_hot(row, 8, unit, none), axis=0))
    pairs = [jnp.concatenate(ones[j:j + 2], axis=1) for j in range(0, blocks, 2)]
    count = jnp.zeros((RANGES, LANES), jnp.float32)
    left = []
    right = []
    for v in range(0, len(pairs), BATCH):
        batch = pairs[v:v + BATCH]
        seen_all = lax.dot_general(jnp.concatenate(batch, axis=0), upto, NN, preferred_element_type=jnp.float32)
        for w in range(len(batch)):
            seen = seen_all[w * RANGES:(w + 1) * RANGES]
            for h in range(2):
                j = 2 * (v + w) + h
                mine = ones[j].astype(jnp.float32)
                before = seen[:, h * LANES:(h + 1) * LANES] + count
                rank = jnp.sum(mine * before, axis=0, keepdims=True) - 1.0
                upper = rank >= LANES // 2
                rank = bf16_rows(jnp.where(upper, rank - LANES // 2, rank))
                upper = bf16_rows(jnp.where(upper, 1.0, 0.0)) > none
                high = bf16_rows(high_s[pl.ds(j, 1), :])
                low = bf16_rows(low_s[pl.ds(j, 1), :])
                sign = bf16_rows(sign_s[pl.ds(j, 1), :])
                same = [first + jnp.bfloat16(16 * k) == rank for k in range(4)]
                left.append(jnp.concatenate(
                    [jnp.where(m, value, none) for value in (high, low, sign) for m in same], axis=0))
                parts = [ones[j][16 * k:16 * k + 16] for k in range(8)]
                right.append(jnp.concatenate(
                    [jnp.where(upper, none, part) for part in parts] + [jnp.where(upper, part, none) for part in parts],
                    axis=0))
            count = count + jnp.broadcast_to(seen[:, wide - 1:wide], (RANGES, LANES))
    placed = jnp.zeros((3 * LANES // 2, 2 * RANGES), jnp.float32)
    for v in range(0, blocks, CHUNK):
        placed = placed + lax.dot_general(
            jnp.concatenate(left[v:v + CHUNK], axis=1), jnp.concatenate(right[v:v + CHUNK], axis=1), NT,
            preferred_element_type=jnp.float32)

    def slots(c):
        rows = placed[c * LANES // 2:(c + 1) * LANES // 2]
        return jnp.concatenate([rows[:, :RANGES], rows[:, RANGES:]], axis=0)

    full = jnp.max(jnp.where(count > CAP, 1.0, 0.0), axis=0, keepdims=True)
    full = jnp.max(full, axis=1, keepdims=True)

    slot = iota((LANES, RANGES), 0)
    real = slot < CAP
    high = slots(0)
    low = slots(1)
    sign = jnp.where(real, slots(2), 0.0)
    pos = jnp.maximum(sign, 0.0)
    neg = jnp.maximum(-sign, 0.0)
    p0 = iota((RANGES, RANGES), 0)
    p1 = iota((RANGES, RANGES), 1)
    r0 = ((p0 & 31) << 2) | (p0 >> 5)
    r1 = ((p1 & 31) << 2) | (p1 >> 5)
    above = (r0 > r1).astype(jnp.bfloat16)
    both = jnp.concatenate([pos, neg], axis=0).astype(jnp.bfloat16)
    later = lax.dot_general(both, above, NN, preferred_element_type=jnp.float32)
    for c, own in ((1, pos), (2, neg)):
        higher = jnp.sum(later[(c - 1) * LANES:c * LANES], axis=0, keepdims=True)
        total = jnp.sum(jnp.sum(own, axis=0, keepdims=True), axis=1, keepdims=True)
        sent = jnp.where(real, own, jnp.where(slot == CAP, higher, total))
        out_ref[pl.ds(c, RANGES, stride=3), :] = sent.T
    out_ref[pl.ds(0, RANGES, stride=3), :] = jnp.where(real, LANES * high + low, full).T


def in_three(x):
    first = x.astype(jnp.bfloat16)
    rest = x - first.astype(jnp.float32)
    second = rest.astype(jnp.bfloat16)
    rest = rest - second.astype(jnp.float32)
    return first, second, rest.astype(jnp.bfloat16)


def curve_kernel(in_ref, curve_ref, part_ref, fix_ref, flag_ref):
    none = jnp.zeros((16, LANES), jnp.bfloat16)
    unit = jnp.ones((16, LANES), jnp.bfloat16)
    first = iota((16, LANES), 0).astype(jnp.float32).astype(jnp.bfloat16)
    real = iota((16, LANES), 1) < CAP
    left = []
    right = []
    for q in range(RANGES):
        place = in_ref[pl.ds(3 * q, 1), :]
        high = jnp.floor(place * (1.0 / LANES))
        low = bf16_rows(place - LANES * high)
        high = bf16_rows(high)
        pos = jnp.where(real, jnp.broadcast_to(in_ref[pl.ds(3 * q + 1, 1), :], (16, LANES)), 0.0).astype(jnp.bfloat16)
        neg = jnp.where(real, jnp.broadcast_to(in_ref[pl.ds(3 * q + 2, 1), :], (16, LANES)), 0.0).astype(jnp.bfloat16)
        same = [first + jnp.bfloat16(16 * k) == high for k in range(4)]
        left.append(jnp.concatenate(
            [jnp.where(m, pos, none) for m in same] + [jnp.where(m, neg, none) for m in same], axis=0))
        right.append(jnp.concatenate(one_hot(low, 8, unit, none), axis=0))
    hist = lax.dot_general(jnp.concatenate(left, axis=1), jnp.concatenate(right, axis=1), NT,
                           preferred_element_type=jnp.float32)
    sums = in_ref[pl.ds(0, 24), :]
    for q in range(24, 3 * RANGES, 24):
        sums = sums + in_ref[pl.ds(q, 24), :]
    kind = iota((24, LANES), 0) % 3
    sums = [jnp.sum(jnp.where(kind == c, sums, 0.0), axis=0, keepdims=True) for c in range(3)]
    flag = sums[0][:, CAP:CAP + 1]
    higher_pos = sums[1][:, CAP:CAP + 1]
    total_pos = sums[1][:, CAP + 1:CAP + 2]
    higher_neg = sums[2][:, CAP:CAP + 1]
    total_neg = sums[2][:, CAP + 1:CAP + 2]
    upper = (iota((LANES, LANES), 0) >= iota((LANES, LANES), 1)).astype(jnp.bfloat16)
    row = iota((2 * ROWS, 2 * ROWS), 0)
    col = iota((2 * ROWS, 2 * ROWS), 1)
    below = ((col > row) & ((col >= ROWS) == (row >= ROWS))).astype(jnp.bfloat16)
    pieces = in_three(hist)
    in_row = lax.dot_general(jnp.concatenate(pieces, axis=1), jnp.concatenate([upper] * 3, axis=0), NN,
                             preferred_element_type=jnp.float32)
    rows_after = lax.dot_general(jnp.concatenate([below] * 3, axis=1), jnp.concatenate(pieces, axis=0), NN,
                                 preferred_element_type=jnp.float32)
    cumulative = in_row + jnp.sum(rows_after, axis=1, keepdims=True)
    true_pos = cumulative[:ROWS] + higher_pos
    false_pos = cumulative[ROWS:] + higher_neg
    pos_hist = hist[:ROWS]
    neg_hist = hist[ROWS:]
    precision = true_pos / jnp.maximum(true_pos + false_pos, 1.0)
    curve_ref[0] = true_pos / total_pos
    curve_ref[1] = precision
    roc = jnp.sum(neg_hist * (2.0 * true_pos - pos_hist), axis=0, keepdims=True)
    prc = jnp.sum(pos_hist * precision, axis=0, keepdims=True)
    roc = jnp.sum(roc, axis=1, keepdims=True) / (2.0 * total_pos * total_neg)
    prc = jnp.sum(prc, axis=1, keepdims=True) / total_pos
    lane = iota((RANGES, 1, LANES), 2)
    part_ref[...] = jnp.where(lane == 0, roc[None], jnp.where(lane == 1, prc[None], flag[None]))
    fix_ref[...] = jnp.zeros((8, LANES), jnp.float32)
    flag_ref[0] = jnp.max(flag)


def join_kernel(own_ref, two_ref, one_ref, three_ref, tpr_ref, precision_ref):
    me = lax.axis_index("grp")
    for k, ref in enumerate((own_ref, one_ref, two_ref, three_ref)):
        source = (me - k) & 3
        tpr_ref[source] = ref[0]
        precision_ref[source] = ref[1]


def area_kernel(part_ref, fix_ref, roc_ref, prc_ref, fix_s, done):
    sums = jnp.sum(part_ref[...].reshape(RANGES, LANES), axis=0, keepdims=True)
    lane = iota((1, LANES), 1)
    roc_ref[0] = jnp.sum(jnp.where(lane == 0, sums, 0.0))
    prc_ref[0] = jnp.sum(jnp.where(lane == 1, sums, 0.0))

    @pl.when(jnp.sum(jnp.where(lane == 2, sums, 0.0)) > 0.0)
    def _():
        copy = pltpu.make_async_copy(fix_ref, fix_s, done)
        copy.start()
        copy.wait()
        fix = fix_s[0:1, :]
        roc_ref[0] = jnp.sum(jnp.where(lane == 0, fix, 0.0))
        prc_ref[0] = jnp.sum(jnp.where(lane == 1, fix, 0.0))


def vmem():
    return pl.BlockSpec(memory_space=pltpu.VMEM)


def smem():
    return pl.BlockSpec(memory_space=pltpu.SMEM)


def f32(*shape):
    return jax.ShapeDtypeStruct(shape, jnp.float32)


def near(*shape):
    return pltpu.VMEM(shape, jnp.float32)


def at_hand(x):
    return pltpu.with_memory_space_constraint(x, pltpu.VMEM)


def on_device(bucket, label, group, group_weight):
    blocks = bucket.shape[0] // LANES
    message = pl.pallas_call(
        route_kernel,
        out_shape=near(3 * RANGES, LANES),
        in_specs=[smem(), vmem(), vmem(), vmem()],
        out_specs=vmem(),
        scratch_shapes=[pltpu.VMEM((blocks, LANES), jnp.float32)] * 4,
        name="route",
    )(group_weight, bucket.reshape(blocks, LANES), label.reshape(blocks, LANES), group.reshape(blocks, LANES))
    received = lax.all_to_all(message.reshape(RANGES, 1, 3 * LANES), AXES, 0, 0, tiled=True)
    curves, parts, fix, flag = pl.pallas_call(
        curve_kernel,
        out_shape=(near(2, ROWS, LANES), near(RANGES, 1, LANES), f32(8, LANES), f32(1)),
        in_specs=[vmem()],
        out_specs=(vmem(), vmem(), vmem(), smem()),
        name="curve",
    )(at_hand(received.reshape(3 * RANGES, LANES)))
    parts = lax.all_to_all(parts, AXES, 0, 0, tiled=True)
    others = [lax.ppermute(curves, "grp", [(i, (i + k) % 4) for i in range(4)]) for k in (2, 1, 3)]
    tpr, precision = pl.pallas_call(
        join_kernel,
        out_shape=(f32(4, ROWS, LANES), f32(4, ROWS, LANES)),
        in_specs=[vmem()] * 4,
        out_specs=(vmem(), vmem()),
        name="join",
    )(at_hand(curves), *[at_hand(x) for x in others])
    size = 4 * ROWS * LANES

    def again(state):
        nothing = (state[0] < 0.0).astype(jnp.int32)
        tpr, precision, roc, prc = general(bucket + nothing, label + nothing, group + nothing, group_weight)
        fix = jnp.where(jnp.arange(LANES)[None, :] == 0, roc, prc)
        return jnp.zeros((), jnp.float32), jnp.broadcast_to(fix, (8, LANES)), tpr, precision

    _, fix, tpr, precision = lax.while_loop(
        lambda state: state[0] > 0.0, again,
        (flag.reshape(()), fix, tpr.reshape(size), precision.reshape(size)))
    roc, prc = pl.pallas_call(
        area_kernel,
        out_shape=(f32(1), f32(1)),
        in_specs=[vmem(), pl.BlockSpec(memory_space=pl.ANY)],
        out_specs=(smem(), smem()),
        scratch_shapes=[pltpu.VMEM((8, LANES), jnp.float32), pltpu.SemaphoreType.DMA],
        name="area",
    )(at_hand(parts), fix)
    return tpr, precision, roc.reshape(()), prc.reshape(())


def solution(mesh):
    placed = (P(AXES), P(AXES), P(AXES), P())
    return jax.shard_map(
        on_device,
        mesh=mesh,
        in_specs=placed,
        out_specs=(P("shard"), P("shard"), P(), P()),
        check_vma=False,
    )
```
